32 devices in a mesh: hst: 4 (over y, x), chip: 8 (over z, core).
Axes of the slice: x: 2, y: 2, z: 4, core: 2. Of those that a mesh axis runs over, the one named last changes fastest.
Arguments:
- resident_row_blocks: bfloat16 [1536, 128, 128], P(('hst', 'chip')), may hold values from -3 to 3
- orphan_blocks: bfloat16 [1024, 128, 128], P(('hst', 'chip')), may hold values from -3 to 3
- home_offsets: int32 [1536, 32, 8], P(('hst', 'chip')), may hold values from 0 to 127
- home_lengths: int32 [1536, 32], P(('hst', 'chip')), may hold values from 1 to 8
- home_samples: int32 [1536, 32], P(('hst', 'chip')), may hold values from 0 to 511
- orphan_offsets: int32 [1024, 32, 8], P(('hst', 'chip')), may hold values from 0 to 127
- orphan_lengths: int32 [1024, 32], P(('hst', 'chip')), may hold values from 1 to 8
- orphan_samples: int32 [1024, 32], P(('hst', 'chip')), may hold values from 0 to 511
- orphan_owner: int32 [1024, 1], P(('hst', 'chip')), may hold values from 0 to 7; in each aligned block of 32 rows (0 to 31, 32 to 63, ...) at most 8 rows name the same one
- dense_inputs: bfloat16 [16384, 13], P(('hst', 'chip')), may hold values from -6 to 6
- labels: int32 [16384], P(('hst', 'chip')), may hold values 0 or 1
- bottom_first: bfloat16 [13, 512], replicated, may hold values from -1.75 to 1.75
- bias_first: float32 [512], replicated, may hold values from -1.5 to 1.5
- bottom_second: bfloat16 [512, 256], replicated, may hold values from -0.375 to 0.375
- bias_second: float32 [256], replicated, may hold values from -1.5 to 1.5
- bottom_third: bfloat16 [256, 128], replicated, may hold values from -0.5 to 0.5
- bias_third: float32 [128], replicated, may hold values from -1.5 to 1.5
- top_hidden: bfloat16 [479, 1024], replicated, may hold values from -0.125 to 0.125
- bias_hidden: float32 [1024], replicated, may hold values from -1.5 to 1.5
- top_logit: bfloat16 [1024, 1], replicated, may hold values from -0.25 to 0.25
- bias_logit: float32 [1], replicated, may hold values from -3 to 3
Outputs:
- rehomed: bfloat16 [2048, 128, 128], P(('hst', 'chip'))
- logits: float32 [16384], P(('hst', 'chip'))
- loss: float32 [], replicated
The draws below stay inside these ranges and needn't reach their ends.
Inputs may be any that keep to these rules, and one draw needn't show every extreme that they name: `orphan_owner`: among the 32 orphans of one device at most 8 have the same new owner; some holder and owner reach 8.
All inputs are finite; a program needn't handle non-finite values. No bound on the sum of `labels` on one device may be relied on, other than what follows from the above.
Results may differ from the reference program's by a relative error of at most 0.0079.
Values may be sent and summed in bfloat16 or wider, within the bound.
A program may use at most 128 MiB of HBM per device.

```python
import math
import jax
import jax.numpy as jnp
import numpy as np
from jax import lax

E = 128
F = 26
DENSE = 13
BOT1 = 512
BOT2 = 256
TOP1 = 1024
BR = 128
L = 8
ORPH_DEV = 32
BATCH_DEV = 512
SLOT = 8
RECV = 64
PIECES = 32
RESIDENT = 1536
ORPHANS = 1024
BATCH = 16384
INTER = 479
N_HST = 4
N_CHIP = 8
DEVICES = 32


def touch_ends(result, stream_key, low, high):
    shape = result.shape
    index_at = [jax.random.randint(jax.random.fold_in(stream_key, axis), (), 0, shape[axis]) for axis in range(len(shape))]
    result = result.at[tuple(index_at)].set(low)
    longest = shape.index(max(shape))
    index_at[longest] = (index_at[longest] + 1) % shape[longest]
    return result.at[tuple(index_at)].set(high)


def levels(rng, dims, cuts, low, top_value):
    loudness = 1.0
    for position, blocks in cuts:
        steps = jax.random.uniform(jax.random.fold_in(jax.random.fold_in(rng, 6), position), (blocks,), jnp.float32, low / len(cuts), top_value / len(cuts))
        loudness = loudness * jnp.repeat(jnp.exp(steps), dims[position] // blocks).reshape((-1,) + (1,) * (len(dims) - 1 - position))
    return loudness


def shared_out(own_key, own, number, rows, number_of, top, bound, slope):
    ranking = jax.random.permutation(own_key, number_of)
    heavy_load, ordinary = portions_of(number_of, rows * top, bound, slope, True), portions_of(number_of, rows * top, bound, slope, False)
    places = jnp.arange(number_of)

    def named(tallies, turn):
        used = int((tallies > 0).sum())
        fixed = max(1, used // 4)
        shifted = fixed + (places - fixed + turn * (used - fixed)) % max(1, number_of - fixed)
        return jnp.zeros((number_of,), jnp.int32).at[ranking[jnp.where(places < fixed, places, shifted)]].set(jnp.asarray(tallies, jnp.int32))

    tallies = jnp.where(number % 4 == 0, named(heavy_load, number // 4), named(ordinary, number - number // 4 - 1))
    mixed = jax.random.permutation(jax.random.fold_in(own, 3), number_of)
    donor, taker = mixed[0:number_of // 2 * 2:2], mixed[1:number_of // 2 * 2:2]
    slack = jnp.minimum(tallies[donor] - 1, bound - tallies[taker]) // 2
    slack = jnp.where((donor == ranking[0]) | (taker == ranking[0]) | (tallies[taker] == 0), 0, jnp.maximum(slack, 0))
    shifted = jax.random.randint(jax.random.fold_in(own, 4), (number_of // 2,), 0, 1 << 20) % (slack + 1)
    tallies = tallies.at[donor].add(-shifted).at[taker].add(shifted)
    items = jnp.searchsorted(jnp.cumsum(tallies), jnp.arange(rows * top), side="right").astype(jnp.int32)
    listing = items.reshape(top, rows).T
    listing = listing[jax.random.permutation(jax.random.fold_in(own, 1), rows)]
    turn = jax.random.randint(jax.random.fold_in(own, 2), (rows, 1), 0, top)
    return jnp.take_along_axis(listing, (jnp.arange(top)[None, :] + turn) % top, axis=1)


def portions_of(count, total, limit, slope, full):
    portions = [(1 << 20) // math.isqrt(standing ** slope) + 1 for standing in range(1, count + 1)]
    largest = limit if full else min(limit, max(-(-total // count), total * portions[0] // sum(portions)))
    least = 1 if total - largest >= count - 1 else 0
    given, surplus = [largest] + [least] * (count - 1), total - largest - least * (count - 1)
    while surplus > 0:
        candidates = [i for i in range(1, count) if given[i] < largest] or [i for i in range(1, count) if given[i] < limit]
        mass, remaining = sum([portions[i] for i in candidates]), surplus
        for i in candidates:
            addition = min(limit - given[i], max(1, remaining * portions[i] // mass), surplus)
            given[i] = given[i] + addition
            surplus = surplus - addition
    return np.array(given)


def gaussian(key, dims, scale, reach, split=(), held_as=jnp.bfloat16):
    values = jax.random.normal(key, dims, jnp.float32) * scale
    if len(split) > 0:
        values = levels(key, dims, split, -0.22, 0.18) * values
    return jnp.clip(values, min=-reach, max=reach).astype(held_as)


def setup_inputs(seed: int = 0) -> dict:
    seeds = jax.random.split(jax.random.key(seed), 22)
    resident_row_blocks = gaussian(seeds[0], (RESIDENT, BR, E), 0.5, 3.0, ((0, 32),))
    orphan_blocks = gaussian(seeds[1], (ORPHANS, BR, E), 0.5, 3.0, ((0, 32),))
    home_offsets = touch_ends(jax.random.randint(seeds[2], (RESIDENT, PIECES, L), 0, BR), jax.random.fold_in(seeds[2], 1), 0, BR - 1).astype(jnp.int32)
    home_lengths = touch_ends(jax.random.randint(seeds[3], (RESIDENT, PIECES), 1, L + 1), jax.random.fold_in(seeds[3], 1), 1, L).astype(jnp.int32)
    home_samples = touch_ends(jax.random.randint(seeds[4], (RESIDENT, PIECES), 0, BATCH_DEV), jax.random.fold_in(seeds[4], 1), 0, BATCH_DEV - 1).astype(jnp.int32)
    orphan_offsets = touch_ends(jax.random.randint(seeds[5], (ORPHANS, PIECES, L), 0, BR), jax.random.fold_in(seeds[5], 1), 0, BR - 1).astype(jnp.int32)
    orphan_lengths = touch_ends(jax.random.randint(seeds[6], (ORPHANS, PIECES), 1, L + 1), jax.random.fold_in(seeds[6], 1), 1, L).astype(jnp.int32)
    orphan_samples = touch_ends(jax.random.randint(seeds[7], (ORPHANS, PIECES), 0, BATCH_DEV), jax.random.fold_in(seeds[7], 1), 0, BATCH_DEV - 1).astype(jnp.int32)
    orphan_owner_keys = jax.random.split(jax.random.fold_in(seeds[8], 1), ORPHANS // ORPH_DEV)
    orphan_owner_turns = jax.random.permutation(jax.random.fold_in(seeds[8], 3), ORPHANS // ORPH_DEV)
    orphan_owner = jax.vmap(lambda own, number: shared_out(jax.random.fold_in(seeds[8], 2), own, number, ORPH_DEV, N_CHIP, 1, SLOT, 2))(orphan_owner_keys, orphan_owner_turns).reshape((ORPHANS, 1))
    dense_inputs = gaussian(seeds[9], (BATCH, DENSE), 1.0, 6.0, ((0, 32),))
    labels = touch_ends((jax.random.randint(seeds[10], (BATCH,), 0, 2) < 1).astype(jnp.int32), jax.random.fold_in(seeds[10], 1), 0, 1)
    bottom_first = gaussian(seeds[11], (DENSE, BOT1), DENSE ** -0.5, 1.75)
    bias_first = gaussian(seeds[12], (BOT1,), 0.3, 1.5, (), jnp.float32)
    bottom_second = gaussian(seeds[13], (BOT1, BOT2), (BOT1 // 2) ** -0.5, 0.375)
    bias_second = gaussian(seeds[14], (BOT2,), 0.3, 1.5, (), jnp.float32)
    bottom_third = gaussian(seeds[15], (BOT2, E), (BOT2 // 2) ** -0.5, 0.5)
    bias_third = gaussian(seeds[16], (E,), 0.3, 1.5, (), jnp.float32)
    top_hidden = gaussian(seeds[17], (INTER, TOP1), (INTER * 4) ** -0.5, 0.125)
    bias_hidden = gaussian(seeds[18], (TOP1,), 0.3, 1.5, (), jnp.float32)
    top_logit = gaussian(seeds[19], (TOP1, 1), (TOP1 // 2) ** -0.5, 0.25)
    bias_logit = gaussian(seeds[20], (1,), 1.0, 3.0, (), jnp.float32)
    return dict(resident_row_blocks=resident_row_blocks, orphan_blocks=orphan_blocks, home_offsets=home_offsets, home_lengths=home_lengths, home_samples=home_samples, orphan_offsets=orphan_offsets, orphan_lengths=orphan_lengths, orphan_samples=orphan_samples, orphan_owner=orphan_owner, dense_inputs=dense_inputs, labels=labels, bottom_first=bottom_first, bias_first=bias_first, bottom_second=bottom_second, bias_second=bias_second, bottom_third=bottom_third, bias_third=bias_third, top_hidden=top_hidden, bias_hidden=bias_hidden, top_logit=top_logit, bias_logit=bias_logit)


def pool_one(block, offsets, lengths):
    rows = jnp.arange(block.shape[0], dtype=jnp.int32)
    places = jnp.arange(offsets.shape[1], dtype=jnp.int32)
    hit = (offsets[:, :, None] == rows[None, None, :]) & (places[None, :, None] < lengths[:, None, None])
    counts = jnp.sum(hit.astype(jnp.float32), axis=1)
    return jnp.dot(counts.astype(jnp.bfloat16), block, preferred_element_type=jnp.float32).astype(jnp.bfloat16)


def slot_provenance(owners):
    count = owners.shape[0]
    index = jnp.arange(count, dtype=jnp.int32)
    earlier = index[None, :] < index[:, None]
    rank = jnp.sum(((owners[:, None] == owners[None, :]) & earlier).astype(jnp.int32), axis=1).astype(jnp.int32)
    flat = owners * SLOT + rank
    match = flat[None, :] == jnp.arange(RECV, dtype=jnp.int32)[:, None]
    source = jnp.sum(match.astype(jnp.int32) * index[None, :], axis=1).astype(jnp.int32)
    return source, jnp.any(match, axis=1)


def reference(resident_row_blocks, orphan_blocks, home_offsets, home_lengths, home_samples, orphan_offsets, orphan_lengths, orphan_samples, orphan_owner, dense_inputs, labels, bottom_first, bias_first, bottom_second, bias_second, bottom_third, bias_third, top_hidden, bias_hidden, top_logit, bias_logit):
    grouped = orphan_blocks.reshape(DEVICES, ORPH_DEV, BR, E)
    owners = orphan_owner[:, 0].reshape(DEVICES, ORPH_DEV)

    def outgoing(blocks, targets):
        source, filled = slot_provenance(targets)
        return jnp.where(filled[:, None, None], blocks[source], jnp.zeros((), jnp.bfloat16))

    buffers = jax.vmap(outgoing)(grouped, owners)
    buffers = buffers.reshape(N_HST, N_CHIP, N_CHIP, SLOT, BR, E).transpose(0, 2, 1, 3, 4, 5)
    rehomed = buffers.reshape(DEVICES * RECV, BR, E)

    blocks = jnp.concatenate([resident_row_blocks, orphan_blocks], axis=0)
    offsets = jnp.concatenate([home_offsets, orphan_offsets], axis=0)
    lengths = jnp.concatenate([home_lengths, orphan_lengths], axis=0)
    samples = jnp.concatenate([home_samples, orphan_samples], axis=0)
    ids = jnp.arange(blocks.shape[0], dtype=jnp.int32)
    feature = ids % F
    piece = lax.map(lambda item: pool_one(item[0], item[1], item[2]), (blocks, offsets, lengths))
    owner = jnp.arange(PIECES, dtype=jnp.int32)
    target = (owner[None, :] * BATCH_DEV + samples) * F + feature[:, None]
    pooled = jax.ops.segment_sum(piece.reshape(-1, E).astype(jnp.float32), target.reshape(-1).astype(jnp.int32), num_segments=BATCH * F)
    pooled = pooled.reshape(BATCH, F, E)

    first = jax.nn.relu(jnp.dot(dense_inputs, bottom_first, preferred_element_type=jnp.float32) + bias_first).astype(jnp.bfloat16)
    second = jax.nn.relu(jnp.dot(first, bottom_second, preferred_element_type=jnp.float32) + bias_second).astype(jnp.bfloat16)
    bottom = jax.nn.relu(jnp.dot(second, bottom_third, preferred_element_type=jnp.float32) + bias_third)
    stacked_vectors = jnp.concatenate([bottom[:, None, :], pooled], axis=1).astype(jnp.bfloat16)
    widened_features = stacked_vectors.astype(jnp.float32)
    pairwise_products = jnp.einsum("asu,adu->asd", widened_features, widened_features)
    lower_i, lower_j = np.tril_indices(F + 1, -1)
    pairs = pairwise_products[:, lower_i, lower_j]
    feature_vectors = jnp.concatenate([bottom, pairs], axis=1).astype(jnp.bfloat16)
    hidden = jax.nn.relu(jnp.dot(feature_vectors, top_hidden, preferred_element_type=jnp.float32) + bias_hidden).astype(jnp.bfloat16)
    logits = jnp.dot(hidden, top_logit, preferred_element_type=jnp.float32)[:, 0] + bias_logit[0]
    loss = jnp.sum(jax.nn.softplus(logits) - labels.astype(jnp.float32) * logits)
    return rehomed, logits, loss
```

```python
import functools

import jax
import jax.numpy as jnp
from jax import lax
from jax.experimental import pallas as pl
from jax.experimental.pallas import tpu as pltpu
from jax.sharding import PartitionSpec as P

F = 26
CORES = 2
CHUNKS = 3
SLAB = 32
VM, HBM, SMEM = pltpu.VMEM, pltpu.HBM, pltpu.SMEM
F32, BF16, I32 = jnp.float32, jnp.bfloat16, jnp.int32
MESH = pl.DeviceIdType.MESH


def cost(flops, bytes_accessed):
    return pl.CostEstimate(flops=flops, bytes_accessed=bytes_accessed, transcendentals=0)


def nt(a, b):
    return lax.dot_general(a, b, (((1,), (1,)), ((), ())), preferred_element_type=F32)


def mm(a, b):
    return jnp.dot(a, b, preferred_element_type=F32)


def turn(j, half):
    if j >= half - CORES:
        return 0, half - 1 - j
    return 1 + j // CORES, j % CORES


def walk(chip, half, side, a, b):
    per = half // CORES
    base, local = lax.div(chip, half), lax.rem(chip, half)
    base = lax.rem(base + side, 2) * half
    return base + lax.rem(lax.div(local, CORES) + a, per) * CORES + lax.rem(local + b, CORES)


NAMES = (
    "owner", "orph", "home", "hoff", "ooff", "hlen", "olen", "hsamp", "osamp",
    "dense", "w1", "b1", "w2", "b2", "w3", "b3", "wt", "bh", "wl", "label",
)


def step_kernel(hosts, chips, slots, cap, depth, *refs):
    half = chips // 2
    devices = hosts * chips
    bl_ref = refs[0]
    hbm = dict(zip(NAMES, refs[1:1 + len(NAMES)]))
    refs = refs[1 + len(NAMES):]
    rehomed, logit_ref, loss_ref, over_ref = refs[:4]
    v = dict(zip(NAMES, refs[4:4 + len(NAMES)]))
    (packed, relay, held, fwd, meta_send, meta, stage, counts, rows, out_rows, arrived, pieces, slab, gram, wpad, wexp,
     order, loss_send, losses,
     in_sems, meta_s, meta_r, row_s, row_r, loss_s, loss_r, list_s, list_r, near_s, near_r, fwd_s, fwd_r,
     own_sems) = refs[4 + len(NAMES):]

    homes, height = v["home"].shape[0], v["home"].shape[1]
    orphs = v["orph"].shape[0]
    count = homes + orphs
    total = devices * count
    width = v["home"].shape[2]
    batch = logit_ref.shape[1]
    part = cap // CHUNKS

    host, chip = lax.axis_index("hst"), lax.axis_index("chip")
    me = host * chips + chip
    mirror = lax.rem(chip + half, chips)

    def peer(e):
        side, e = lax.div(e, hosts * half), lax.rem(e, hosts * half)
        dh, e = lax.div(e, half), lax.rem(e, half)
        return lax.rem(host + dh, hosts), walk(chip, half, side, lax.div(e, CORES), lax.rem(e, CORES))

    bar = pltpu.get_barrier_semaphore()

    def hello(e, carry):
        pl.semaphore_signal(bar, 1, device_id=peer(e), device_id_type=MESH)
        return carry

    lax.fori_loop(1, devices, hello, 0)

    loads = {n: pltpu.make_async_copy(hbm[n], v[n], in_sems.at[k]) for k, n in enumerate(NAMES)}
    for n in NAMES:
        loads[n].start()

    def everyone(src, dst, send, recv, indexed):
        def copy(e):
            h, c = peer(e)
            return pltpu.make_async_remote_copy(
                src_ref=src.at[h * chips + c] if indexed else src.at[0],
                dst_ref=dst.at[me], send_sem=send.at[e], recv_sem=recv.at[e],
                device_id=(h, c), device_id_type=MESH)

        def start():
            def go(i, carry):
                copy(devices - i).start()
                return carry
            lax.fori_loop(1, devices, go, 0)

        def wait(kind):
            def go(i, carry):
                c = copy(devices - i)
                c.wait_recv() if kind == "recv" else c.wait_send()
                return carry
            lax.fori_loop(1, devices, go, 0)

        return start, wait

    meta_go, meta_wait = everyone(meta_send, meta, meta_s, meta_r, True)
    rows_go, rows_wait = everyone(out_rows, arrived, row_s, row_r, True)
    loss_go, loss_wait = everyone(loss_send, losses, loss_s, loss_r, False)

    lists = [
        pltpu.make_async_remote_copy(
            src_ref=packed.at[pl.ds(half * slots + k * part, part)],
            dst_ref=relay.at[pl.ds(k * part, part)],
            send_sem=list_s.at[k], recv_sem=list_r.at[k], device_id=(host, mirror), device_id_type=MESH)
        for k in range(CHUNKS)
    ]

    def group(src, holder, j, send, recv):
        return pltpu.make_async_remote_copy(
            src_ref=src.at[pl.ds(j * slots, slots)],
            dst_ref=rehomed.at[pl.ds(holder * slots, slots)],
            send_sem=send.at[j], recv_sem=recv.at[j],
            device_id=(host, walk(chip, half, 0, *turn(j, half))), device_id_type=MESH)

    near = [group(packed, chip, j, near_s, near_r) for j in range(half - 1)]
    onward = [group(fwd, mirror, j, fwd_s, fwd_r) for j in range(half - 1)]
    own = [
        pltpu.make_async_copy(ref.at[pl.ds((half - 1) * slots, slots)],
                              rehomed.at[pl.ds(holder * slots, slots)], own_sems.at[k])
        for k, (ref, holder) in enumerate(((packed, chip), (fwd, mirror)))
    ]

    loads["owner"].wait()
    to = v["owner"][...]
    key = jnp.zeros_like(to)
    for side in range(2):
        for j in range(half):
            key = jnp.where(to == walk(chip, half, side, *turn(j, half)), side * half + j, key)
    tag = lax.broadcasted_iota(I32, to.shape, 1)
    square = (orphs, orphs)
    code = jnp.broadcast_to((key * orphs + tag).astype(F32), square)
    kind = jnp.broadcast_to(key.astype(F32), square)
    rank = jnp.sum((code.T < code).astype(F32), axis=0, keepdims=True).astype(I32)
    prefix = jnp.sum((kind.T < kind).astype(F32), axis=0, keepdims=True).astype(I32)
    inside = jnp.sum((kind.T < half).astype(F32), axis=0, keepdims=True).astype(I32)
    place = jnp.where(key < half, key * slots + rank - prefix, half * slots + rank - inside)
    sizes = [jnp.sum((key == half + j).astype(I32)) for j in range(half)]
    sizes.append(jnp.sum((key >= half).astype(I32)))
    loads["orph"].wait()

    def pack(first_at, number):
        for t in range(first_at, first_at + number):
            found = jnp.sum(jnp.where(place == t, tag + 1, 0))
            block = v["orph"][jnp.maximum(found - 1, 0)]
            packed[t] = jnp.where(found > 0, block, jnp.zeros_like(block))

    pack(half * slots, part)
    pl.semaphore_wait(bar, devices - 1)
    lists[0].start()
    pack(0, half * slots)
    near[half - CORES].start()
    near[0].start()
    own[0].start()
    pack(half * slots + part, cap - part)

    stage[...] = jnp.zeros_like(stage)
    loads["osamp"].wait()
    stage[0:orphs, 0:devices] = v["osamp"][...].astype(F32)
    turned = stage[...].T[0:devices].astype(I32)
    lane = lax.broadcasted_iota(I32, (devices, 128), 1)
    rest = pltpu.roll(turned, homes, 1)
    loads["hsamp"].wait()
    stage[0:devices, 0:homes] = v["hsamp"][...].astype(F32)
    line = jnp.where(lane < homes, stage[0:devices].astype(I32), rest)
    for j in range(half + 1):
        line = jnp.where(lane == count + j, sizes[j], line)
    for p in range(devices):
        meta_send[p] = line[p:p + 1]
    meta[me] = meta_send[me]

    meta_go()

    row = lax.broadcasted_iota(I32, (height, 128), 0)
    bag = hbm["hoff"].shape[1]

    def hits(off):
        found = jnp.zeros((height, 128), F32)
        for k in range(bag):
            found = found + (row == off[k:k + 1]).astype(F32)
        return found.T

    for n in ("hoff", "hlen"):
        loads[n].wait()
    slot = lax.broadcasted_iota(I32, (bag, homes), 0)
    blank = jnp.full((bag, 64 - homes), height, I32)

    def pair(g, carry):
        off = []
        for k in range(2):
            p = g * 2 + k
            off += [jnp.where(slot < v["hlen"][pl.ds(p, 1), :], v["hoff"][p], height), blank]
        found = hits(jnp.concatenate(off, axis=1))
        for k in range(2):
            counts[pl.ds(pl.multiple_of((g * 2 + k) * homes, 8), homes), :] = found[k * 64:k * 64 + homes]
        return carry

    lax.fori_loop(0, devices // 2, pair, 0)
    loads["home"].wait()

    def home_piece(b, carry):
        lhs = counts[pl.ds(b, devices, stride=homes), :].astype(BF16)
        rows[pl.ds(b, devices, stride=count), :] = mm(lhs, v["home"][b])
        return carry

    lax.fori_loop(0, homes, home_piece, 0, unroll=4)
    for n in ("ooff", "olen"):
        loads[n].wait()
    per = 128 // devices
    spot = lax.broadcasted_iota(I32, (bag, devices), 0)

    def orph_group(g, carry):
        off = []
        for k in range(per):
            b = g * per + k
            off.append(jnp.where(spot < v["olen"][pl.ds(b, 1), :], v["ooff"][b], height))
        found = hits(jnp.concatenate(off, axis=1) if per > 1 else off[0]).astype(BF16)
        for k in range(per):
            b = g * per + k
            rows[pl.ds(homes + b, devices, stride=count), :] = mm(found[k * devices:(k + 1) * devices], v["orph"][b])
        return carry

    lax.fori_loop(0, orphs // per, orph_group, 0)
    out_rows[...] = rows[...].reshape(out_rows.shape).astype(BF16)
    rows_go()
    arrived[me] = out_rows[me]
    for j in range(1, half - CORES):
        near[j].start()
    for k in range(1, CHUNKS):
        lists[k].start()
    for j in range(half - CORES + 1, half - 1):
        near[j].start()

    for n in NAMES[9:]:
        loads[n].wait()
    inter = v["wt"].shape[0]
    whole = inter // 16 * 16
    wpad[whole:, :] = jnp.zeros((wpad.shape[0] - whole, wpad.shape[1]), BF16)
    wpad[0:inter, :] = v["wt"][...]
    cell = lax.broadcasted_iota(I32, (SLAB * SLAB, wpad.shape[0]), 0)
    i, j = cell // SLAB, cell % SLAB
    column = lax.broadcasted_iota(I32, cell.shape, 1)
    pick = (column == 128 + i * (i - 1) // 2 + j) & (j < i) & (i <= F)
    wexp[...] = mm(jnp.where(pick, 1.0, 0.0).astype(BF16), wpad[...]).astype(BF16)

    first = lax.dot_general(v["dense"][...], v["w1"][...], (((0,), (0,)), ((), ())), preferred_element_type=F32)
    first = jnp.maximum(first + v["b1"][...], 0.0).astype(BF16)
    second = jnp.maximum(mm(first, v["w2"][...]) + v["b2"][...], 0.0).astype(BF16)
    slab[0] = jnp.maximum(mm(second, v["w3"][...]) + v["b3"][...], 0.0)
    slab[F + 1:] = jnp.zeros((SLAB - F - 1,) + slab.shape[1:], F32)

    meta_wait("recv")
    bits = meta[host * chips + mirror]
    here = lax.broadcasted_iota(I32, bits.shape, 1)
    tops = [jnp.sum(jnp.where(here == count + k, bits, 0)) for k in range(half)]

    def forward(j):
        first_at = sum(tops[:j]) if j else 0

        def go(s, carry):
            at = jnp.minimum(first_at + s, cap - 1)
            fwd[j * slots + s] = jnp.where(s < tops[j], held[at], jnp.zeros(held.shape[1:], BF16))
            return carry

        lax.fori_loop(0, slots, go, 0)
        if j < half - 1:
            onward[j].start()
        else:
            own[1].start()

    def last_chunk(j):
        return (min(cap, (j + 1) * slots) - 1) // part

    at_lane = lax.broadcasted_iota(I32, (1, 128), 1)
    for d in range(depth):
        values = jnp.full((1, 128), -1, I32)
        n = d * F
        while n < min((d + 1) * F, total):
            if n < devices * homes:
                p, s = n // homes, n % homes
                size = homes - s
            else:
                p, s = (n - devices * homes) // orphs, (n - devices * homes) % orphs
                size = orphs - s
                s = homes + s
            to = n - d * F
            size = min(size, F - to)
            moved = pltpu.roll(meta[p], (to - s) % 128, 1) if to != s else meta[p]
            values = jnp.where((at_lane >= to) & (at_lane < to + size), moved, values)
            n += size
        order[d:d + 1, :] = values.astype(F32)
    where = order[...].T[0:SLAB].astype(I32)

    def unpack(k):
        lists[k].wait_recv()
        held[k * part:(k + 1) * part] = relay[k * part:(k + 1) * part]
        for j in range(half):
            if last_chunk(j) == k:
                forward(j)

    unpack(0)

    pieces[total:, :] = jnp.zeros((pieces.shape[0] - total, pieces.shape[1]), F32)
    rows_wait("recv")

    def settle(p, carry):
        pieces[pl.ds(pl.multiple_of(p * homes, 8), homes), :] = arrived[p, 0:homes].astype(F32)
        pieces[pl.ds(pl.multiple_of(devices * homes + p * orphs, 8), orphs), :] = (
            arrived[p, homes:count].astype(F32))
        return carry

    lax.fori_loop(0, devices, settle, 0, unroll=2)

    sample = lax.broadcasted_iota(I32, (batch, depth), 0)
    for f in range(F):
        mine = pieces[pl.ds(f, depth, stride=F), :].astype(BF16)
        hot = jnp.where(sample == where[f:f + 1, :], 1.0, 0.0).astype(BF16)
        slab[f + 1] = mm(hot, mine)

    edge = SLAB * 8
    same = (lax.broadcasted_iota(I32, (edge, edge), 0) % 8) == (
        lax.broadcasted_iota(I32, (edge, edge), 1) % 8)

    def products(g, carry):
        halves = []
        for k in range(2):
            at = pl.ds(pl.multiple_of(g * 16 + k * 8, 8), 8)
            x = slab[:, at, :].reshape(edge, slab.shape[2]).astype(BF16)
            halves.append(jnp.where(same, nt(x, x), 0.0).reshape(SLAB, 8, edge))
        both = jnp.concatenate(halves, axis=1).astype(BF16)
        gram[:, pl.ds(pl.multiple_of(g * 16, 16), 16), :] = both
        return carry

    lax.fori_loop(0, batch // 16, products, 0, unroll=2)

    lane_j = lax.broadcasted_iota(I32, (edge, edge), 0) // 8
    out_lane = lax.broadcasted_iota(I32, (edge, edge), 1)
    features = []
    for h in range(SLAB // 8):
        acc = None
        for k in range(8):
            i_ = h * 8 + k
            if i_ < 1 or i_ > F:
                continue
            live = 128 if i_ <= 16 else edge
            fold_ = jnp.where(lane_j + k * SLAB == out_lane, 1.0, 0.0).astype(BF16)
            term = mm(gram[i_, :, 0:live], fold_[0:live])
            acc = term if acc is None else acc + term
        features.append(acc.astype(BF16))
    bottom = slab[0].astype(BF16)

    tally = jnp.zeros((batch, 128), F32)
    step = 256
    scale = v["wl"][...].astype(F32)
    for n in range(0, wpad.shape[1], step):
        pre = mm(bottom, wpad[0:128, n:n + step])
        for h in range(SLAB // 8):
            pre = pre + mm(features[h], wexp[h * 256:(h + 1) * 256, n:n + step])
        hidden = jnp.maximum(pre + v["bh"][:, n:n + step], 0.0).astype(BF16).astype(F32)
        scaled = hidden * scale[:, n:n + step]
        tally = tally + scaled[:, 0:128] + scaled[:, 128:256]
    logits = jnp.sum(tally.T, axis=0, keepdims=True) + bl_ref[0]
    logit_ref[...] = logits
    soft = jnp.maximum(logits, 0.0) + jnp.log1p(jnp.exp(-jnp.abs(logits)))
    loss = jnp.sum(soft - v["label"][...].astype(F32) * logits, axis=1, keepdims=True)
    loss_send[0] = jnp.broadcast_to(loss, (1, 128))
    losses[me] = loss_send[0]
    loss_go()

    for k in range(1, CHUNKS):
        unpack(k)

    crossing = jnp.where(at_lane == count + half, jnp.max(meta[...].astype(F32), axis=0), 0.0)
    over_ref[0] = (jnp.max(crossing) > cap).astype(I32)
    loss_wait("recv")
    loss_ref[0] = jnp.sum(jnp.where(at_lane == 0, jnp.sum(losses[...], axis=0), 0.0))

    meta_wait("send")
    rows_wait("send")
    loss_wait("send")
    for c in lists:
        c.wait_send()
    for c in near + onward:
        c.wait()
    for c in own:
        c.wait()


def step(hosts, chips, slots, bl, arrays):
    devices = hosts * chips
    half = chips // 2
    home, orph = arrays["home"], arrays["orph"]
    homes, height, width = home.shape
    orphs = orph.shape[0]
    count = homes + orphs
    batch = arrays["dense"].shape[1]
    top = arrays["wt"].shape[1]
    cap = -(-3 * orphs // (4 * CHUNKS)) * CHUNKS
    total = devices * count
    depth = -(-total // (F * 128)) * 128
    dma = pltpu.SemaphoreType.DMA
    scratch = [VM(arrays[n].shape, arrays[n].dtype) for n in NAMES] + [
        VM((half * slots + cap, height, width), BF16),
        VM((cap, height, width), BF16),
        VM((cap, height, width), BF16),
        VM((half * slots, height, width), BF16),
        VM((devices, 1, 128), I32),
        VM((devices, 1, 128), I32),
        VM((128, 128), F32),
        VM((devices * homes, height), F32),
        VM((devices * count, width), F32),
        VM((devices, count, width), BF16),
        VM((devices, count, width), BF16),
        VM((F * depth, width), F32),
        VM((SLAB, batch, width), F32),
        VM((SLAB, batch, SLAB * 8), BF16),
        VM((512, top), BF16),
        VM((SLAB * SLAB, top), BF16),
        VM((depth, 128), F32),
        VM((1, 1, 128), F32),
        VM((devices, 1, 128), F32),
        dma((len(NAMES),)),
        dma((devices,)), dma((devices,)), dma((devices,)), dma((devices,)), dma((devices,)), dma((devices,)),
        dma((CHUNKS,)), dma((CHUNKS,)),
        dma((half,)), dma((half,)), dma((half,)), dma((half,)),
        dma((2,)),
    ]
    smem, hbm, vmem = (pl.BlockSpec(memory_space=m) for m in (SMEM, HBM, VM))
    return pl.pallas_call(
        functools.partial(step_kernel, hosts, chips, slots, cap, depth),
        out_shape=(
            jax.ShapeDtypeStruct((chips * slots, height, width), BF16),
            jax.ShapeDtypeStruct((1, batch), F32),
            jax.ShapeDtypeStruct((1,), F32),
            jax.ShapeDtypeStruct((1,), I32),
        ),
        in_specs=[smem] + [hbm] * len(NAMES),
        out_specs=(hbm, vmem, smem, smem),
        scratch_shapes=scratch,
        cost_estimate=cost(8_000_000_000, 8_000_000),
        compiler_params=pltpu.CompilerParams(
            collective_id=0, has_side_effects=True, vmem_limit_bytes=56 * 2**20),
        name="step",
    )(bl, *[arrays[n] for n in NAMES])


def padded(owners, blocks, chips, slots):
    number = blocks.shape[0]
    index = jnp.arange(number, dtype=I32)
    earlier = index[None, :] < index[:, None]
    rank = jnp.sum(((owners[:, None] == owners[None, :]) & earlier).astype(I32), axis=1)
    match = (owners * slots + rank)[None, :] == jnp.arange(chips * slots, dtype=I32)[:, None]
    source = jnp.sum(match.astype(I32) * index[None, :], axis=1)
    filled = jnp.any(match, axis=1)
    groups = jnp.where(filled[:, None, None], blocks[source], jnp.zeros((), BF16))
    return lax.all_to_all(groups, "chip", split_axis=0, concat_axis=0, tiled=True)


def per_device(
    resident_row_blocks,
    orphan_blocks,
    home_offsets,
    home_lengths,
    home_samples,
    orphan_offsets,
    orphan_lengths,
    orphan_samples,
    orphan_owner,
    dense_inputs,
    labels,
    bottom_first,
    bias_first,
    bottom_second,
    bias_second,
    bottom_third,
    bias_third,
    top_hidden,
    bias_hidden,
    top_logit,
    bias_logit,
):
    hosts, chips = lax.axis_size("hst"), lax.axis_size("chip")
    orphs = orphan_blocks.shape[0]
    slots = (2 * orphs + chips - 1) // chips
    owners = orphan_owner[:, 0]
    arrays = dict(
        owner=orphan_owner.T, home=resident_row_blocks, orph=orphan_blocks,
        hoff=home_offsets.transpose(1, 2, 0), ooff=orphan_offsets.transpose(0, 2, 1),
        hlen=home_lengths.T, olen=orphan_lengths, hsamp=home_samples.T, osamp=orphan_samples,
        dense=dense_inputs.T, w1=bottom_first, b1=bias_first[None], w2=bottom_second, b2=bias_second[None],
        w3=bottom_third, b3=bias_third[None], wt=top_hidden, bh=bias_hidden[None], wl=top_logit.T,
        label=labels[None],
    )
    rehomed, logits, loss, over = step(hosts, chips, slots, bias_logit, arrays)
    rehomed = lax.cond(
        over[0] > 0,
        lambda r, o, b: padded(o, b, chips, slots),
        lambda r, o, b: r,
        rehomed, owners, orphan_blocks,
    )
    return rehomed, logits[0], loss[0]


def solution(mesh):
    both = ("hst", "chip")
    three, two = P(both, None, None), P(both, None)
    return jax.shard_map(
        per_device,
        mesh=mesh,
        in_specs=(three, three, three, two, two, three, two, two, two, two, P(both)) + (P(),) * 10,
        out_specs=(three, P(both), P()),
        check_vma=False,
    )
```

```python
import functools

import jax
import jax.numpy as jnp
from jax import lax
from jax.experimental import pallas as pl
from jax.experimental.pallas import tpu as pltpu
from jax.sharding import PartitionSpec as P

F = 26
CORES = 2
PAIR = 2
SLAB = 32
VM, HBM, SMEM = pltpu.VMEM, pltpu.HBM, pltpu.SMEM
F32, BF16, I32 = jnp.float32, jnp.bfloat16, jnp.int32
MESH = pl.DeviceIdType.MESH


def cost(flops, bytes_accessed):
    return pl.CostEstimate(flops=flops, bytes_accessed=bytes_accessed, transcendentals=0)


def nt(a, b):
    return lax.dot_general(a, b, (((1,), (1,)), ((), ())), preferred_element_type=F32)


def mm(a, b):
    return jnp.dot(a, b, preferred_element_type=F32)


def turn(j, half):
    if j >= half - CORES:
        return 0, half - 1 - j
    return 1 + j // CORES, j % CORES


def walk(chip, half, side, a, b):
    per = half // CORES
    base, local = lax.div(chip, half), lax.rem(chip, half)
    base = lax.rem(base + side, 2) * half
    return base + lax.rem(lax.div(local, CORES) + a, per) * CORES + lax.rem(local + b, CORES)


def passes(half, slots, ends):
    found = []
    for j in range(half):
        low = 0
        for k, end in enumerate(ends):
            high = slots if k == len(ends) - 1 else min(slots, end - j * slots)
            if high > low:
                found.append((k, j, low, high))
                low = high
    return sorted(found)


NAMES = (
    "owner", "orph", "home", "hoff", "ooff", "hlen", "olen", "hsamp", "osamp",
    "dense", "w1", "b1", "w2", "b2", "w3", "b3", "wt", "bh", "wl", "label",
)


def step_kernel(hosts, chips, slots, cap, depth, *refs):
    half = chips // 2
    devices = hosts * chips
    bl_ref = refs[0]
    hbm = dict(zip(NAMES, refs[1:1 + len(NAMES)]))
    refs = refs[1 + len(NAMES):]
    rehomed, logit_ref, loss_ref, over_ref = refs[:4]
    v = dict(zip(NAMES, refs[4:4 + len(NAMES)]))
    (packed, relay, held, fwd, meta_send, meta, stage, counts, rows, out_rows, arrived, pieces, slab, gram, wpad, wexp,
     order, loss_send, losses,
     in_sems, meta_s, meta_r, row_s, row_r, loss_s, loss_r, list_s, list_r, near_s, near_r, fwd_s, fwd_r,
     own_sem) = refs[4 + len(NAMES):]

    homes, height = v["home"].shape[0], v["home"].shape[1]
    orphs = v["orph"].shape[0]
    count = homes + orphs
    total = devices * count
    width = v["home"].shape[2]
    batch = logit_ref.shape[1]
    quarter = orphs // 8
    ends = [2 * quarter, 3 * quarter, 4 * quarter, cap]
    starts = [0] + ends[:-1]
    steps = len(ends)

    host, chip = lax.axis_index("hst"), lax.axis_index("chip")
    me = host * chips + chip
    my_half = lax.div(chip, half)
    local, core = lax.div(lax.rem(chip, half), CORES), lax.rem(chip, CORES)
    low_chip = lax.div(local, PAIR) * PAIR
    gate = lax.rem(local, PAIR) == 1 - my_half
    half_chips = half // CORES
    across = (1 - my_half) * half
    target = across + (low_chip + my_half) * CORES + core
    holders = [across + (low_chip + i) * CORES + core for i in range(PAIR)]
    turn_in = lax.rem(local, PAIR)

    def peer(e):
        side, e = lax.div(e, hosts * half), lax.rem(e, hosts * half)
        dh, e = lax.div(e, half), lax.rem(e, half)
        return lax.rem(host + dh, hosts), walk(chip, half, side, lax.div(e, CORES), lax.rem(e, CORES))

    bar = pltpu.get_barrier_semaphore()

    def hello(e, carry):
        pl.semaphore_signal(bar, 1, device_id=peer(e), device_id_type=MESH)
        return carry

    lax.fori_loop(1, devices, hello, 0)

    loads = {n: pltpu.make_async_copy(hbm[n], v[n], in_sems.at[k]) for k, n in enumerate(NAMES)}
    for n in NAMES:
        loads[n].start()

    def everyone(src, dst, send, recv, indexed):
        def copy(e):
            h, c = peer(e)
            return pltpu.make_async_remote_copy(
                src_ref=src.at[h * chips + c] if indexed else src.at[0],
                dst_ref=dst.at[me], send_sem=send.at[e], recv_sem=recv.at[e],
                device_id=(h, c), device_id_type=MESH)

        def start():
            def go(i, carry):
                copy(devices - i).start()
                return carry
            lax.fori_loop(1, devices, go, 0)

        def wait(kind):
            def go(i, carry):
                c = copy(devices - i)
                c.wait_recv() if kind == "recv" else c.wait_send()
                return carry
            lax.fori_loop(1, devices, go, 0)

        return start, wait

    meta_go, meta_wait = everyone(meta_send, meta, meta_s, meta_r, True)
    rows_go, rows_wait = everyone(out_rows, arrived, row_s, row_r, True)
    loss_go, loss_wait = everyone(loss_send, losses, loss_s, loss_r, False)

    lists = [
        pltpu.make_async_remote_copy(
            src_ref=packed.at[pl.ds(half * slots + starts[k], ends[k] - starts[k])],
            dst_ref=relay.at[turn_in, pl.ds(starts[k], ends[k] - starts[k])],
            send_sem=list_s.at[k], recv_sem=list_r.at[turn_in, k],
            device_id=(host, target), device_id_type=MESH)
        for k in range(steps)
    ]

    def listed(i, k):
        size = ends[k] - starts[k]
        return pltpu.make_async_remote_copy(
            src_ref=packed.at[pl.ds(half * slots + starts[k], size)],
            dst_ref=relay.at[i, pl.ds(starts[k], size)],
            send_sem=list_s.at[k], recv_sem=list_r.at[i, k],
            device_id=(host, target), device_id_type=MESH)

    def group(src, holder, j, low, high, send, recv):
        return pltpu.make_async_remote_copy(
            src_ref=src.at[pl.ds(j * slots + low, high - low)],
            dst_ref=rehomed.at[pl.ds(holder * slots + low, high - low)],
            send_sem=send, recv_sem=recv,
            device_id=(host, walk(chip, half, 0, *turn(j, half))), device_id_type=MESH)

    near = [group(packed, chip, j, 0, slots, near_s.at[j], near_r.at[j]) for j in range(half - 1)]
    onward = {}
    for n, (k, j, low, high) in enumerate(passes(half, slots, ends)):
        for i in range(PAIR):
            if j < half - 1:
                onward[i, k, j] = group(fwd.at[i], holders[i], j, low, high, fwd_s.at[i, n], fwd_r.at[i, n])
            else:
                onward[i, k, j] = pltpu.make_async_copy(
                    fwd.at[i, pl.ds(j * slots + low, high - low)],
                    rehomed.at[pl.ds(holders[i] * slots + low, high - low)], fwd_s.at[i, n])
    own = pltpu.make_async_copy(packed.at[pl.ds((half - 1) * slots, slots)],
                                rehomed.at[pl.ds(chip * slots, slots)], own_sem)

    loads["owner"].wait()
    to = v["owner"][...]
    key = jnp.zeros_like(to)
    for side in range(2):
        for j in range(half):
            owner = walk(target if side else chip, half, 0, *turn(j, half))
            key = jnp.where(to == owner, side * half + j, key)
    tag = lax.broadcasted_iota(I32, to.shape, 1)
    square = (orphs, orphs)
    code = jnp.broadcast_to((key * orphs + tag).astype(F32), square)
    kind = jnp.broadcast_to(key.astype(F32), square)
    rank = jnp.sum((code.T < code).astype(F32), axis=0, keepdims=True).astype(I32)
    prefix = jnp.sum((kind.T < kind).astype(F32), axis=0, keepdims=True).astype(I32)
    inside = jnp.sum((kind.T < half).astype(F32), axis=0, keepdims=True).astype(I32)
    place = jnp.where(key < half, key * slots + rank - prefix, half * slots + rank - inside)
    sizes = [jnp.sum((key == half + j).astype(I32)) for j in range(half)]
    sizes.append(jnp.sum((key >= half).astype(I32)))
    loads["orph"].wait()

    def pack(first_at, number):
        for t in range(first_at, first_at + number):
            found = jnp.sum(jnp.where(place == t, tag + 1, 0))
            block = v["orph"][jnp.maximum(found - 1, 0)]
            packed[t] = jnp.where(found > 0, block, jnp.zeros_like(block))

    pack(half * slots, ends[0])
    pl.semaphore_wait(bar, devices - 1)
    lists[0].start()
    pack(half * slots + starts[1], ends[1] - starts[1])
    lists[1].start()
    pack(0, half * slots)
    near[0].start()
    for j in range(half - CORES, half - 1):
        near[j].start()
    own.start()
    pack(half * slots + starts[2], cap - starts[2])

    stage[...] = jnp.zeros_like(stage)
    loads["osamp"].wait()
    stage[0:orphs, 0:devices] = v["osamp"][...].astype(F32)
    turned = stage[...].T[0:devices].astype(I32)
    lane = lax.broadcasted_iota(I32, (devices, 128), 1)
    rest = pltpu.roll(turned, homes, 1)
    loads["hsamp"].wait()
    stage[0:devices, 0:homes] = v["hsamp"][...].astype(F32)
    line = jnp.where(lane < homes, stage[0:devices].astype(I32), rest)
    for j in range(half + 1):
        line = jnp.where(lane == count + j, sizes[j], line)
    for p in range(devices):
        meta_send[p] = line[p:p + 1]
    meta[me] = meta_send[me]

    meta_go()

    row = lax.broadcasted_iota(I32, (height, 128), 0)
    bag = hbm["hoff"].shape[1]

    def hits(off):
        found = jnp.zeros((height, 128), F32)
        for k in range(bag):
            found = found + (row == off[k:k + 1]).astype(F32)
        return found.T

    for n in ("hoff", "hlen"):
        loads[n].wait()
    slot = lax.broadcasted_iota(I32, (bag, homes), 0)
    blank = jnp.full((bag, 64 - homes), height, I32)

    def pair(g, carry):
        off = []
        for k in range(2):
            p = g * 2 + k
            off += [jnp.where(slot < v["hlen"][pl.ds(p, 1), :], v["hoff"][p], height), blank]
        found = hits(jnp.concatenate(off, axis=1))
        for k in range(2):
            counts[pl.ds(pl.multiple_of((g * 2 + k) * homes, 8), homes), :] = found[k * 64:k * 64 + homes]
        return carry

    lax.fori_loop(0, devices // 2, pair, 0)
    loads["home"].wait()

    def home_piece(b, carry):
        lhs = counts[pl.ds(b, devices, stride=homes), :].astype(BF16)
        rows[pl.ds(b, devices, stride=count), :] = mm(lhs, v["home"][b])
        return carry

    lax.fori_loop(0, homes, home_piece, 0, unroll=4)
    for n in ("ooff", "olen"):
        loads[n].wait()
    per = 128 // devices
    spot = lax.broadcasted_iota(I32, (bag, devices), 0)

    def orph_group(g, carry):
        off = []
        for k in range(per):
            b = g * per + k
            off.append(jnp.where(spot < v["olen"][pl.ds(b, 1), :], v["ooff"][b], height))
        found = hits(jnp.concatenate(off, axis=1) if per > 1 else off[0]).astype(BF16)
        for k in range(per):
            b = g * per + k
            rows[pl.ds(homes + b, devices, stride=count), :] = mm(found[k * devices:(k + 1) * devices], v["orph"][b])
        return carry

    lax.fori_loop(0, orphs // per, orph_group, 0)
    out_rows[...] = rows[...].reshape(out_rows.shape).astype(BF16)
    rows_go()
    arrived[me] = out_rows[me]
    for k in range(2, steps):
        lists[k].start()
    for j in range(1, half - CORES):
        near[j].start()

    for n in NAMES[9:]:
        loads[n].wait()
    inter = v["wt"].shape[0]
    whole = inter // 16 * 16
    wpad[whole:, :] = jnp.zeros((wpad.shape[0] - whole, wpad.shape[1]), BF16)
    wpad[0:inter, :] = v["wt"][...]
    cell = lax.broadcasted_iota(I32, (SLAB * SLAB, wpad.shape[0]), 0)
    i, j = cell // SLAB, cell % SLAB
    column = lax.broadcasted_iota(I32, cell.shape, 1)
    pick = (column == 128 + i * (i - 1) // 2 + j) & (j < i) & (i <= F)
    wexp[...] = mm(jnp.where(pick, 1.0, 0.0).astype(BF16), wpad[...]).astype(BF16)

    first = lax.dot_general(v["dense"][...], v["w1"][...], (((0,), (0,)), ((), ())), preferred_element_type=F32)
    first = jnp.maximum(first + v["b1"][...], 0.0).astype(BF16)
    second = jnp.maximum(mm(first, v["w2"][...]) + v["b2"][...], 0.0).astype(BF16)
    slab[0] = jnp.maximum(mm(second, v["w3"][...]) + v["b3"][...], 0.0)
    slab[F + 1:] = jnp.zeros((SLAB - F - 1,) + slab.shape[1:], F32)

    meta_wait("recv")
    def unpack(k):
        size = ends[k] - starts[k]
        for i in range(PAIR):
            listed(i, k).wait_recv()
            held[i, starts[k]:ends[k]] = relay[i, starts[k]:ends[k]]
            bits = meta[host * chips + holders[i]]
            here = lax.broadcasted_iota(I32, bits.shape, 1)
            for step_, j, low, high in passes(half, slots, ends):
                if step_ != k:
                    continue
                first_at = jnp.sum(jnp.where((here >= count) & (here < count + j), bits, 0))
                number = jnp.sum(jnp.where(here == count + j, bits, 0))

                def go(s, carry):
                    at = jnp.minimum(first_at + s, cap - 1)
                    block = held[i, at]
                    fwd[i, j * slots + s] = jnp.where(s < number, block, jnp.zeros_like(block))
                    return carry

                lax.fori_loop(low, high, go, 0)
                onward[i, k, j].start()

    at_lane = lax.broadcasted_iota(I32, (1, 128), 1)
    for d in range(depth):
        values = jnp.full((1, 128), -1, I32)
        n = d * F
        while n < min((d + 1) * F, total):
            if n < devices * homes:
                p, s = n // homes, n % homes
                size = homes - s
            else:
                p, s = (n - devices * homes) // orphs, (n - devices * homes) % orphs
                size = orphs - s
                s = homes + s
            to = n - d * F
            size = min(size, F - to)
            moved = pltpu.roll(meta[p], (to - s) % 128, 1) if to != s else meta[p]
            values = jnp.where((at_lane >= to) & (at_lane < to + size), moved, values)
            n += size
        order[d:d + 1, :] = values.astype(F32)
    where = order[...].T[0:SLAB].astype(I32)

    @pl.when(gate)
    def _():
        unpack(0)
        unpack(1)

    pieces[total:, :] = jnp.zeros((pieces.shape[0] - total, pieces.shape[1]), F32)
    rows_wait("recv")

    def settle(p, carry):
        pieces[pl.ds(pl.multiple_of(p * homes, 8), homes), :] = arrived[p, 0:homes].astype(F32)
        pieces[pl.ds(pl.multiple_of(devices * homes + p * orphs, 8), orphs), :] = (
            arrived[p, homes:count].astype(F32))
        return carry

    lax.fori_loop(0, devices, settle, 0, unroll=2)

    sample = lax.broadcasted_iota(I32, (batch, depth), 0)
    for f in range(F):
        mine = pieces[pl.ds(f, depth, stride=F), :].astype(BF16)
        hot = jnp.where(sample == where[f:f + 1, :], 1.0, 0.0).astype(BF16)
        slab[f + 1] = mm(hot, mine)

    edge = SLAB * 8
    same = (lax.broadcasted_iota(I32, (edge, edge), 0) % 8) == (
        lax.broadcasted_iota(I32, (edge, edge), 1) % 8)

    def products(g, carry):
        halves = []
        for k in range(2):
            at = pl.ds(pl.multiple_of(g * 16 + k * 8, 8), 8)
            x = slab[:, at, :].reshape(edge, slab.shape[2]).astype(BF16)
            halves.append(jnp.where(same, nt(x, x), 0.0).reshape(SLAB, 8, edge))
        both = jnp.concatenate(halves, axis=1).astype(BF16)
        gram[:, pl.ds(pl.multiple_of(g * 16, 16), 16), :] = both
        return carry

    lax.fori_loop(0, batch // 16, products, 0, unroll=2)

    @pl.when(gate)
    def _():
        unpack(2)

    lane_j = lax.broadcasted_iota(I32, (edge, edge), 0) // 8
    out_lane = lax.broadcasted_iota(I32, (edge, edge), 1)
    features = []
    for h in range(SLAB // 8):
        acc = None
        for k in range(8):
            i_ = h * 8 + k
            if i_ < 1 or i_ > F:
                continue
            live = 128 if i_ <= 16 else edge
            fold_ = jnp.where(lane_j + k * SLAB == out_lane, 1.0, 0.0).astype(BF16)
            term = mm(gram[i_, :, 0:live], fold_[0:live])
            acc = term if acc is None else acc + term
        features.append(acc.astype(BF16))
    bottom = slab[0].astype(BF16)

    tally = jnp.zeros((batch, 128), F32)
    step = 256
    scale = v["wl"][...].astype(F32)
    for n in range(0, wpad.shape[1], step):
        pre = mm(bottom, wpad[0:128, n:n + step])
        for h in range(SLAB // 8):
            pre = pre + mm(features[h], wexp[h * 256:(h + 1) * 256, n:n + step])
        hidden = jnp.maximum(pre + v["bh"][:, n:n + step], 0.0).astype(BF16).astype(F32)
        scaled = hidden * scale[:, n:n + step]
        tally = tally + scaled[:, 0:128] + scaled[:, 128:256]
    logits = jnp.sum(tally.T, axis=0, keepdims=True) + bl_ref[0]
    logit_ref[...] = logits
    soft = jnp.maximum(logits, 0.0) + jnp.log1p(jnp.exp(-jnp.abs(logits)))
    loss = jnp.sum(soft - v["label"][...].astype(F32) * logits, axis=1, keepdims=True)
    loss_send[0] = jnp.broadcast_to(loss, (1, 128))
    losses[me] = loss_send[0]
    loss_go()

    @pl.when(gate)
    def _():
        unpack(3)

    crossing = jnp.where(at_lane == count + half, jnp.max(meta[...].astype(F32), axis=0), 0.0)
    over_ref[0] = (jnp.max(crossing) > cap).astype(I32)
    loss_wait("recv")
    loss_ref[0] = jnp.sum(jnp.where(at_lane == 0, jnp.sum(losses[...], axis=0), 0.0))

    meta_wait("send")
    rows_wait("send")
    loss_wait("send")
    for c in lists:
        c.wait_send()
    for c in near:
        c.wait()
    own.wait()

    @pl.when(gate)
    def _():
        for k, j, low, high in passes(half, slots, ends):
            for i in range(PAIR):
                onward[i, k, j].wait_send() if j < half - 1 else onward[i, k, j].wait()

    for k, j, low, high in passes(half, slots, ends):
        if j == half - 1:
            continue
        source = lax.rem(local - turn(j, half)[0] + half_chips, half_chips)

        @pl.when(lax.rem(source, PAIR) == 1 - my_half)
        def _():
            for i in range(PAIR):
                onward[i, k, j].wait_recv()


def step(hosts, chips, slots, bl, arrays):
    devices = hosts * chips
    half = chips // 2
    home, orph = arrays["home"], arrays["orph"]
    homes, height, width = home.shape
    orphs = orph.shape[0]
    count = homes + orphs
    batch = arrays["dense"].shape[1]
    top = arrays["wt"].shape[1]
    cap = -(-11 * orphs // 16)
    total = devices * count
    depth = -(-total // (F * 128)) * 128
    dma = pltpu.SemaphoreType.DMA
    scratch = [VM(arrays[n].shape, arrays[n].dtype) for n in NAMES] + [
        VM((half * slots + cap, height, width), BF16),
        VM((PAIR, cap, height, width), BF16),
        VM((PAIR, cap, height, width), BF16),
        VM((PAIR, half * slots, height, width), BF16),
        VM((devices, 1, 128), I32),
        VM((devices, 1, 128), I32),
        VM((128, 128), F32),
        VM((devices * homes, height), F32),
        VM((devices * count, width), F32),
        VM((devices, count, width), BF16),
        VM((devices, count, width), BF16),
        VM((F * depth, width), F32),
        VM((SLAB, batch, width), F32),
        VM((SLAB, batch, SLAB * 8), BF16),
        VM((512, top), BF16),
        VM((SLAB * SLAB, top), BF16),
        VM((depth, 128), F32),
        VM((1, 1, 128), F32),
        VM((devices, 1, 128), F32),
        dma((len(NAMES),)),
        dma((devices,)), dma((devices,)), dma((devices,)), dma((devices,)), dma((devices,)), dma((devices,)),
        dma((4,)), dma((PAIR, 4)),
        dma((half,)), dma((half,)), dma((PAIR, 2 * half + 4)), dma((PAIR, 2 * half + 4)),
        dma,
    ]
    smem, hbm, vmem = (pl.BlockSpec(memory_space=m) for m in (SMEM, HBM, VM))
    return pl.pallas_call(
        functools.partial(step_kernel, hosts, chips, slots, cap, depth),
        out_shape=(
            jax.ShapeDtypeStruct((chips * slots, height, width), BF16),
            jax.ShapeDtypeStruct((1, batch), F32),
            jax.ShapeDtypeStruct((1,), F32),
            jax.ShapeDtypeStruct((1,), I32),
        ),
        in_specs=[smem] + [hbm] * len(NAMES),
        out_specs=(hbm, vmem, smem, smem),
        scratch_shapes=scratch,
        cost_estimate=cost(8_000_000_000, 8_000_000),
        compiler_params=pltpu.CompilerParams(
            collective_id=0, has_side_effects=True, vmem_limit_bytes=56 * 2**20),
        name="step",
    )(bl, *[arrays[n] for n in NAMES])


def padded(owners, blocks, chips, slots):
    number = blocks.shape[0]
    index = jnp.arange(number, dtype=I32)
    earlier = index[None, :] < index[:, None]
    rank = jnp.sum(((owners[:, None] == owners[None, :]) & earlier).astype(I32), axis=1)
    match = (owners * slots + rank)[None, :] == jnp.arange(chips * slots, dtype=I32)[:, None]
    source = jnp.sum(match.astype(I32) * index[None, :], axis=1)
    filled = jnp.any(match, axis=1)
    groups = jnp.where(filled[:, None, None], blocks[source], jnp.zeros((), BF16))
    return lax.all_to_all(groups, "chip", split_axis=0, concat_axis=0, tiled=True)


def per_device(
    resident_row_blocks,
    orphan_blocks,
    home_offsets,
    home_lengths,
    home_samples,
    orphan_offsets,
    orphan_lengths,
    orphan_samples,
    orphan_owner,
    dense_inputs,
    labels,
    bottom_first,
    bias_first,
    bottom_second,
    bias_second,
    bottom_third,
    bias_third,
    top_hidden,
    bias_hidden,
    top_logit,
    bias_logit,
):
    hosts, chips = lax.axis_size("hst"), lax.axis_size("chip")
    orphs = orphan_blocks.shape[0]
    slots = (2 * orphs + chips - 1) // chips
    owners = orphan_owner[:, 0]
    arrays = dict(
        owner=orphan_owner.T, home=resident_row_blocks, orph=orphan_blocks,
        hoff=home_offsets.transpose(1, 2, 0), ooff=orphan_offsets.transpose(0, 2, 1),
        hlen=home_lengths.T, olen=orphan_lengths, hsamp=home_samples.T, osamp=orphan_samples,
        dense=dense_inputs.T, w1=bottom_first, b1=bias_first[None], w2=bottom_second, b2=bias_second[None],
        w3=bottom_third, b3=bias_third[None], wt=top_hidden, bh=bias_hidden[None], wl=top_logit.T,
        label=labels[None],
    )
    rehomed, logits, loss, over = step(hosts, chips, slots, bias_logit, arrays)
    rehomed = lax.cond(
        over[0] > 0,
        lambda r, o, b: padded(o, b, chips, slots),
        lambda r, o, b: r,
        rehomed, owners, orphan_blocks,
    )
    return rehomed, logits[0], loss[0]


def solution(mesh):
    both = ("hst", "chip")
    three, two = P(both, None, None), P(both, None)
    return jax.shard_map(
        per_device,
        mesh=mesh,
        in_specs=(three, three, three, two, two, three, two, two, two, two, P(both)) + (P(),) * 10,
        out_specs=(three, P(both), P()),
        check_vma=False,
    )
```

```python
import functools

import jax
import jax.numpy as jnp
from jax import lax
from jax.experimental import pallas as pl
from jax.experimental.pallas import tpu as pltpu
from jax.sharding import PartitionSpec as P

F = 26
CORES = 2
PAIR = 2
SLAB = 32
VM, HBM, SMEM = pltpu.VMEM, pltpu.HBM, pltpu.SMEM
F32, BF16, I32 = jnp.float32, jnp.bfloat16, jnp.int32
MESH = pl.DeviceIdType.MESH


def cost(flops, bytes_accessed):
    return pl.CostEstimate(flops=flops, bytes_accessed=bytes_accessed, transcendentals=0)


def nt(a, b):
    return lax.dot_general(a, b, (((1,), (1,)), ((), ())), preferred_element_type=F32)


def mm(a, b):
    return jnp.dot(a, b, preferred_element_type=F32)


def turn(j, half):
    if j >= half - CORES:
        return 0, half - 1 - j
    return 1 + j // CORES, j % CORES


def walk(chip, half, side, a, b):
    per = half // CORES
    base, local = lax.div(chip, half), lax.rem(chip, half)
    base = lax.rem(base + side, 2) * half
    return base + lax.rem(lax.div(local, CORES) + a, per) * CORES + lax.rem(local + b, CORES)


def passes(half, slots, ends):
    found = []
    for j in range(half):
        low = 0
        for k, end in enumerate(ends):
            high = slots if k == len(ends) - 1 else min(slots, end - j * slots)
            if high > low:
                found.append((k, j, low, high))
                low = high
    return sorted(found)


NAMES = (
    "owner", "orph", "home", "hoff", "ooff", "hlen", "olen", "hsamp", "osamp",
    "dense", "w1", "b1", "w2", "b2", "w3", "b3", "wt", "bh", "wl", "label",
)


def step_kernel(hosts, chips, slots, cap, depth, *refs):
    half = chips // 2
    devices = hosts * chips
    bl_ref = refs[0]
    hbm = dict(zip(NAMES, refs[1:1 + len(NAMES)]))
    refs = refs[1 + len(NAMES):]
    rehomed, logit_ref, loss_ref, over_ref = refs[:4]
    v = dict(zip(NAMES, refs[4:4 + len(NAMES)]))
    (packed, relay, held, fwd, meta_send, meta, stage, counts, rows, out_rows, arrived, pieces, slab, gram, wpad, wexp,
     order, loss_send, losses,
     in_sems, meta_s, meta_r, row_s, row_r, loss_s, loss_r, list_s, list_r, near_s, near_r, fwd_s, fwd_r) = refs[4 + len(NAMES):]

    homes, height = v["home"].shape[0], v["home"].shape[1]
    orphs = v["orph"].shape[0]
    count = homes + orphs
    total = devices * count
    width = v["home"].shape[2]
    batch = logit_ref.shape[1]
    quarter = orphs // 8
    ends = [2 * quarter, 3 * quarter, 4 * quarter, cap]
    starts = [0] + ends[:-1]
    steps = len(ends)

    host, chip = lax.axis_index("hst"), lax.axis_index("chip")
    me = host * chips + chip
    my_half = lax.div(chip, half)
    local, core = lax.div(lax.rem(chip, half), CORES), lax.rem(chip, CORES)
    low_chip = lax.div(local, PAIR) * PAIR
    gate = lax.rem(local, PAIR) == 1 - my_half
    half_chips = half // CORES
    across = (1 - my_half) * half
    target = across + (low_chip + my_half) * CORES + core
    holders = [across + (low_chip + i) * CORES + core for i in range(PAIR)]
    turn_in = lax.rem(local, PAIR)

    at_host = [lax.rem(host + dh, hosts) for dh in range(hosts)]
    at_chip = [walk(chip, half, side, k // CORES, k % CORES) for side in range(2) for k in range(half)]
    peers = [(at_host[dh], at_chip[side * half + k])
             for side in range(2) for dh in range(hosts) for k in range(half)]
    others = [(e, *peers[e]) for e in range(devices - 1, 0, -1)]

    loads = {n: pltpu.make_async_copy(hbm[n], v[n], in_sems.at[k]) for k, n in enumerate(NAMES)}
    for n in NAMES[:2]:
        loads[n].start()
    bar = pltpu.get_barrier_semaphore()

    for _, h, c in others:
        pl.semaphore_signal(bar, 1, device_id=(h, c), device_id_type=MESH)
    for n in NAMES[2:]:
        loads[n].start()

    def everyone(src, dst, send, recv, indexed):
        copies = [
            pltpu.make_async_remote_copy(
                src_ref=src.at[h * chips + c] if indexed else src.at[0],
                dst_ref=dst.at[me], send_sem=send.at[e], recv_sem=recv.at[e],
                device_id=(h, c), device_id_type=MESH)
            for e, h, c in others
        ]

        def start():
            for copy in copies:
                copy.start()

        def wait(kind):
            for copy in copies:
                copy.wait_recv() if kind == "recv" else copy.wait_send()

        return start, wait

    meta_go, meta_wait = everyone(meta_send, meta, meta_s, meta_r, True)
    rows_go, rows_wait = everyone(out_rows, arrived, row_s, row_r, True)
    loss_go, loss_wait = everyone(loss_send, losses, loss_s, loss_r, False)

    lists = [
        pltpu.make_async_remote_copy(
            src_ref=packed.at[pl.ds(half * slots + starts[k], ends[k] - starts[k])],
            dst_ref=relay.at[turn_in, pl.ds(starts[k], ends[k] - starts[k])],
            send_sem=list_s.at[k], recv_sem=list_r.at[turn_in, k],
            device_id=(host, target), device_id_type=MESH)
        for k in range(steps)
    ]

    def listed(i, k):
        size = ends[k] - starts[k]
        return pltpu.make_async_remote_copy(
            src_ref=packed.at[pl.ds(half * slots + starts[k], size)],
            dst_ref=relay.at[i, pl.ds(starts[k], size)],
            send_sem=list_s.at[k], recv_sem=list_r.at[i, k],
            device_id=(host, target), device_id_type=MESH)

    def group(src, holder, j, low, high, send, recv):
        return pltpu.make_async_remote_copy(
            src_ref=src.at[pl.ds(j * slots + low, high - low)],
            dst_ref=rehomed.at[pl.ds(holder * slots + low, high - low)],
            send_sem=send, recv_sem=recv,
            device_id=(host, walk(chip, half, 0, *turn(j, half))), device_id_type=MESH)

    near = [group(packed, chip, j, 0, slots, near_s.at[j], near_r.at[j]) for j in range(half - 1)]
    onward = {}
    for n, (k, j, low, high) in enumerate(passes(half, slots, ends)):
        for i in range(PAIR):
            if j < half - 1:
                onward[i, k, j] = group(fwd.at[i], holders[i], j, low, high, fwd_s.at[i, n], fwd_r.at[i, n])

    loads["owner"].wait()
    to = v["owner"][...]
    key = jnp.zeros_like(to)
    for side in range(2):
        for j in range(half):
            owner = walk(target if side else chip, half, 0, *turn(j, half))
            key = jnp.where(to == owner, side * half + j, key)
    tag = lax.broadcasted_iota(I32, to.shape, 1)
    square = (orphs, orphs)
    code = jnp.broadcast_to((key * orphs + tag).astype(F32), square)
    kind = jnp.broadcast_to(key.astype(F32), square)
    rank = jnp.sum((code.T < code).astype(F32), axis=0, keepdims=True).astype(I32)
    prefix = jnp.sum((kind.T < kind).astype(F32), axis=0, keepdims=True).astype(I32)
    inside = jnp.sum((kind.T < half).astype(F32), axis=0, keepdims=True).astype(I32)
    place = jnp.where(key < half, key * slots + rank - prefix, half * slots + rank - inside)
    loads["orph"].wait()

    def pack(first_at, number):
        for t in range(first_at, first_at + number):
            found = jnp.sum(jnp.where(place == t, tag + 1, 0))
            block = v["orph"][jnp.maximum(found - 1, 0)]
            packed[t] = jnp.where(found > 0, block, jnp.zeros_like(block))

    pack(half * slots, ends[0])
    pl.semaphore_wait(bar, devices - 1)
    lists[0].start()
    sizes = [jnp.sum((key == half + j).astype(I32)) for j in range(half)]
    sizes.append(jnp.sum((key >= half).astype(I32)))
    stage[...] = jnp.zeros_like(stage)
    loads["osamp"].wait()
    stage[0:orphs, 0:devices] = v["osamp"][...].astype(F32)
    turned = stage[...].T[0:devices].astype(I32)
    lane = lax.broadcasted_iota(I32, (devices, 128), 1)
    rest = pltpu.roll(turned, homes, 1)
    loads["hsamp"].wait()
    stage[0:devices, 0:homes] = v["hsamp"][...].astype(F32)
    line = jnp.where(lane < homes, stage[0:devices].astype(I32), rest)
    for j in range(half + 1):
        line = jnp.where(lane == count + j, sizes[j], line)
    for p in range(devices):
        meta_send[p] = line[p:p + 1]
    meta[me] = meta_send[me]

    meta_go()

    pack(0, half * slots)
    near[0].start()
    for j in range(half - CORES, half - 1):
        near[j].start()
    rehomed[pl.ds(chip * slots, slots)] = packed[(half - 1) * slots:half * slots]
    pack(half * slots + starts[1], cap - starts[1])

    row = lax.broadcasted_iota(I32, (height, 128), 0)
    bag = hbm["hoff"].shape[1]

    def hits(off):
        found = jnp.zeros((height, 128), F32)
        for k in range(bag):
            found = found + (row == off[k:k + 1]).astype(F32)
        return found.T

    for n in ("hoff", "hlen"):
        loads[n].wait()
    slot = lax.broadcasted_iota(I32, (bag, homes), 0)
    blank = jnp.full((bag, 64 - homes), height, I32)

    def pair(g, carry):
        off = []
        for k in range(2):
            p = g * 2 + k
            off += [jnp.where(slot < v["hlen"][pl.ds(p, 1), :], v["hoff"][p], height), blank]
        found = hits(jnp.concatenate(off, axis=1))
        for k in range(2):
            counts[pl.ds(pl.multiple_of((g * 2 + k) * homes, 8), homes), :] = found[k * 64:k * 64 + homes]
        return carry

    lax.fori_loop(0, devices // 2, pair, 0)
    loads["home"].wait()

    def home_piece(b, carry):
        lhs = counts[pl.ds(b, devices, stride=homes), :].astype(BF16)
        rows[pl.ds(b, devices, stride=count), :] = mm(lhs, v["home"][b])
        return carry

    lax.fori_loop(0, homes, home_piece, 0, unroll=4)
    for n in ("ooff", "olen"):
        loads[n].wait()
    per = 128 // devices
    spot = lax.broadcasted_iota(I32, (bag, devices), 0)

    def orph_group(g, carry):
        off = []
        for k in range(per):
            b = g * per + k
            off.append(jnp.where(spot < v["olen"][pl.ds(b, 1), :], v["ooff"][b], height))
        found = hits(jnp.concatenate(off, axis=1) if per > 1 else off[0]).astype(BF16)
        for k in range(per):
            b = g * per + k
            rows[pl.ds(homes + b, devices, stride=count), :] = mm(found[k * devices:(k + 1) * devices], v["orph"][b])
        return carry

    lax.fori_loop(0, orphs // per, orph_group, 0)
    out_rows[...] = rows[...].reshape(out_rows.shape).astype(BF16)
    rows_go()

    arrived[me] = out_rows[me]

    for n in NAMES[9:]:
        loads[n].wait()
    inter = v["wt"].shape[0]
    whole = inter // 16 * 16
    wpad[whole:, :] = jnp.zeros((wpad.shape[0] - whole, wpad.shape[1]), BF16)
    wpad[0:inter, :] = v["wt"][...]
    cell = lax.broadcasted_iota(I32, (SLAB * SLAB, wpad.shape[0]), 0)
    i, j = cell // SLAB, cell % SLAB
    column = lax.broadcasted_iota(I32, cell.shape, 1)
    pick = (column == 128 + i * (i - 1) // 2 + j) & (j < i) & (i <= F)
    wexp[...] = mm(jnp.where(pick, 1.0, 0.0).astype(BF16), wpad[...]).astype(BF16)

    first = lax.dot_general(v["dense"][...], v["w1"][...], (((0,), (0,)), ((), ())), preferred_element_type=F32)
    first = jnp.maximum(first + v["b1"][...], 0.0).astype(BF16)
    second = jnp.maximum(mm(first, v["w2"][...]) + v["b2"][...], 0.0).astype(BF16)
    slab[0] = jnp.maximum(mm(second, v["w3"][...]) + v["b3"][...], 0.0)
    slab[F + 1:] = jnp.zeros((SLAB - F - 1,) + slab.shape[1:], F32)

    meta_wait("recv")
    def unpack(k):
        size = ends[k] - starts[k]
        for i in range(PAIR):
            listed(i, k).wait_recv()
            held[i, starts[k]:ends[k]] = relay[i, starts[k]:ends[k]]
            bits = meta[host * chips + holders[i]]
            here = lax.broadcasted_iota(I32, bits.shape, 1)
            for step_, j, low, high in passes(half, slots, ends):
                if step_ != k:
                    continue
                first_at = jnp.sum(jnp.where((here >= count) & (here < count + j), bits, 0))
                number = jnp.sum(jnp.where(here == count + j, bits, 0))

                def go(s, carry):
                    at = jnp.minimum(first_at + s, cap - 1)
                    block = held[i, at]
                    block = jnp.where(s < number, block, jnp.zeros_like(block))
                    if j < half - 1:
                        fwd[i, j * slots + s] = block
                    else:
                        rehomed[holders[i] * slots + s] = block
                    return carry

                lax.fori_loop(low, high, go, 0)
                if j < half - 1:
                    onward[i, k, j].start()

    at_lane = lax.broadcasted_iota(I32, (1, 128), 1)
    for d in range(depth):
        values = jnp.full((1, 128), -1, I32)
        n = d * F
        while n < min((d + 1) * F, total):
            if n < devices * homes:
                p, s = n // homes, n % homes
                size = homes - s
            else:
                p, s = (n - devices * homes) // orphs, (n - devices * homes) % orphs
                size = orphs - s
                s = homes + s
            to = n - d * F
            size = min(size, F - to)
            moved = pltpu.roll(meta[p], (to - s) % 128, 1) if to != s else meta[p]
            values = jnp.where((at_lane >= to) & (at_lane < to + size), moved, values)
            n += size
        order[d:d + 1, :] = values.astype(F32)
    where = order[...].T[0:SLAB].astype(I32)

    @pl.when(gate)
    def _():
        unpack(0)

    pieces[total:, :] = jnp.zeros((pieces.shape[0] - total, pieces.shape[1]), F32)
    rows_wait("recv")

    lists[1].start()
    lists[2].start()
    for j in range(1, half - CORES):
        near[j].start()

    def settle(p, carry):
        pieces[pl.ds(pl.multiple_of(p * homes, 8), homes), :] = arrived[p, 0:homes].astype(F32)
        pieces[pl.ds(pl.multiple_of(devices * homes + p * orphs, 8), orphs), :] = (
            arrived[p, homes:count].astype(F32))
        return carry

    lax.fori_loop(0, devices, settle, 0, unroll=2)

    sample = lax.broadcasted_iota(I32, (batch, depth), 0)
    for f in range(F):
        mine = pieces[pl.ds(f, depth, stride=F), :].astype(BF16)
        hot = jnp.where(sample == where[f:f + 1, :], 1.0, 0.0).astype(BF16)
        slab[f + 1] = mm(hot, mine)

    edge = SLAB * 8
    same = (lax.broadcasted_iota(I32, (edge, edge), 0) % 8) == (
        lax.broadcasted_iota(I32, (edge, edge), 1) % 8)

    def products(g, carry):
        halves = []
        for k in range(2):
            at = pl.ds(pl.multiple_of(g * 16 + k * 8, 8), 8)
            x = slab[:, at, :].reshape(edge, slab.shape[2]).astype(BF16)
            halves.append(jnp.where(same, nt(x, x), 0.0).reshape(SLAB, 8, edge))
        both = jnp.concatenate(halves, axis=1).astype(BF16)
        gram[:, pl.ds(pl.multiple_of(g * 16, 16), 16), :] = both
        return carry

    lax.fori_loop(0, batch // 16, products, 0, unroll=2)

    @pl.when(gate)
    def _():
        unpack(1)

    lane_j = lax.broadcasted_iota(I32, (edge, edge), 0) // 8
    out_lane = lax.broadcasted_iota(I32, (edge, edge), 1)
    features = []
    for h in range(SLAB // 8):
        acc = None
        for k in range(8):
            i_ = h * 8 + k
            if i_ < 1 or i_ > F:
                continue
            live = 128 if i_ <= 16 else edge
            fold_ = jnp.where(lane_j + k * SLAB == out_lane, 1.0, 0.0).astype(BF16)
            term = mm(gram[i_, :, 0:live], fold_[0:live])
            acc = term if acc is None else acc + term
        features.append(acc.astype(BF16))
    bottom = slab[0].astype(BF16)

    tally = jnp.zeros((batch, 128), F32)
    step = 256
    scale = v["wl"][...].astype(F32)
    for n in range(0, wpad.shape[1], step):
        pre = mm(bottom, wpad[0:128, n:n + step])
        for h in range(SLAB // 8):
            pre = pre + mm(features[h], wexp[h * 256:(h + 1) * 256, n:n + step])
        hidden = jnp.maximum(pre + v["bh"][:, n:n + step], 0.0).astype(BF16).astype(F32)
        scaled = hidden * scale[:, n:n + step]
        tally = tally + scaled[:, 0:128] + scaled[:, 128:256]
    logits = jnp.sum(tally.T, axis=0, keepdims=True) + bl_ref[0]
    logit_ref[...] = logits
    soft = jnp.maximum(logits, 0.0) + jnp.log1p(jnp.exp(-jnp.abs(logits)))
    loss = jnp.sum(soft - v["label"][...].astype(F32) * logits, axis=1, keepdims=True)
    loss_send[0] = jnp.broadcast_to(loss, (1, 128))
    losses[me] = loss_send[0]
    loss_go()
    lists[3].start()

    @pl.when(gate)
    def _():
        unpack(2)
        unpack(3)

    crossing = jnp.where(at_lane == count + half, jnp.max(meta[...].astype(F32), axis=0), 0.0)
    over_ref[0] = (jnp.max(crossing) > cap).astype(I32)
    loss_wait("recv")
    loss_ref[0] = jnp.sum(jnp.where(at_lane == 0, jnp.sum(losses[...], axis=0), 0.0))

    meta_wait("send")
    rows_wait("send")
    loss_wait("send")
    for c in lists:
        c.wait_send()
    for c in near:
        c.wait()

    @pl.when(gate)
    def _():
        for k, j, low, high in passes(half, slots, ends):
            for i in range(PAIR if j < half - 1 else 0):
                onward[i, k, j].wait_send()

    for k, j, low, high in passes(half, slots, ends):
        if j == half - 1:
            continue
        source = lax.rem(local - turn(j, half)[0] + half_chips, half_chips)

        @pl.when(lax.rem(source, PAIR) == 1 - my_half)
        def _():
            for i in range(PAIR):
                onward[i, k, j].wait_recv()


def step(hosts, chips, slots, bl, arrays):
    devices = hosts * chips
    half = chips // 2
    home, orph = arrays["home"], arrays["orph"]
    homes, height, width = home.shape
    orphs = orph.shape[0]
    count = homes + orphs
    batch = arrays["dense"].shape[1]
    top = arrays["wt"].shape[1]
    cap = -(-3 * orphs // 4)
    total = devices * count
    depth = -(-total // (F * 128)) * 128
    dma = pltpu.SemaphoreType.DMA
    scratch = [VM(arrays[n].shape, arrays[n].dtype) for n in NAMES] + [
        VM((half * slots + cap, height, width), BF16),
        VM((PAIR, cap, height, width), BF16),
        VM((PAIR, cap, height, width), BF16),
        VM((PAIR, half * slots, height, width), BF16),
        VM((devices, 1, 128), I32),
        VM((devices, 1, 128), I32),
        VM((128, 128), F32),
        VM((devices * homes, height), F32),
        VM((devices * count, width), F32),
        VM((devices, count, width), BF16),
        VM((devices, count, width), BF16),
        VM((F * depth, width), F32),
        VM((SLAB, batch, width), F32),
        VM((SLAB, batch, SLAB * 8), BF16),
        VM((512, top), BF16),
        VM((SLAB * SLAB, top), BF16),
        VM((depth, 128), F32),
        VM((1, 1, 128), F32),
        VM((devices, 1, 128), F32),
        dma((len(NAMES),)),
        dma((devices,)), dma((devices,)), dma((devices,)), dma((devices,)), dma((devices,)), dma((devices,)),
        dma((4,)), dma((PAIR, 4)),
        dma((half,)), dma((half,)), dma((PAIR, 2 * half + 4)), dma((PAIR, 2 * half + 4)),
    ]
    smem, hbm, vmem = (pl.BlockSpec(memory_space=m) for m in (SMEM, HBM, VM))
    return pl.pallas_call(
        functools.partial(step_kernel, hosts, chips, slots, cap, depth),
        out_shape=(
            jax.ShapeDtypeStruct((chips * slots, height, width), BF16),
            jax.ShapeDtypeStruct((1, batch), F32),
            jax.ShapeDtypeStruct((1,), F32),
            jax.ShapeDtypeStruct((1,), I32),
        ),
        in_specs=[smem] + [hbm] * len(NAMES),
        out_specs=(vmem, vmem, smem, smem),
        scratch_shapes=scratch,
        cost_estimate=cost(8_000_000_000, 8_000_000),
        compiler_params=pltpu.CompilerParams(
            collective_id=0, has_side_effects=True, vmem_limit_bytes=56 * 2**20),
        name="step",
    )(bl, *[arrays[n] for n in NAMES])


def finish_kernel(parts, rehomed, logits, rehomed_out, logits_out, sems):
    size = rehomed.shape[0] // parts
    copies = [
        pltpu.make_async_copy(rehomed.at[pl.ds(k * size, size)], rehomed_out.at[pl.ds(k * size, size)], sems.at[k])
        for k in range(parts)
    ]
    copies.append(pltpu.make_async_copy(logits, logits_out, sems.at[parts]))
    for copy in copies:
        copy.start()
    for copy in copies:
        copy.wait()


def finish(rehomed, logits, parts=4):
    vmem, hbm = pl.BlockSpec(memory_space=VM), pl.BlockSpec(memory_space=HBM)
    return pl.pallas_call(
        functools.partial(finish_kernel, parts),
        out_shape=(jax.ShapeDtypeStruct(rehomed.shape, rehomed.dtype),
                   jax.ShapeDtypeStruct(logits.shape, logits.dtype)),
        in_specs=[vmem, hbm],
        out_specs=(hbm, hbm),
        scratch_shapes=[pltpu.SemaphoreType.DMA((parts + 1,))],
        cost_estimate=cost(1000, 2 * rehomed.size * 2),
        compiler_params=pltpu.CompilerParams(vmem_limit_bytes=2 * 2**20),
        name="finish",
    )(rehomed, logits)


def padded(owners, blocks, chips, slots):
    number = blocks.shape[0]
    index = jnp.arange(number, dtype=I32)
    earlier = index[None, :] < index[:, None]
    rank = jnp.sum(((owners[:, None] == owners[None, :]) & earlier).astype(I32), axis=1)
    match = (owners * slots + rank)[None, :] == jnp.arange(chips * slots, dtype=I32)[:, None]
    source = jnp.sum(match.astype(I32) * index[None, :], axis=1)
    filled = jnp.any(match, axis=1)
    groups = jnp.where(filled[:, None, None], blocks[source], jnp.zeros((), BF16))
    return lax.all_to_all(groups, "chip", split_axis=0, concat_axis=0, tiled=True)


def per_device(
    resident_row_blocks,
    orphan_blocks,
    home_offsets,
    home_lengths,
    home_samples,
    orphan_offsets,
    orphan_lengths,
    orphan_samples,
    orphan_owner,
    dense_inputs,
    labels,
    bottom_first,
    bias_first,
    bottom_second,
    bias_second,
    bottom_third,
    bias_third,
    top_hidden,
    bias_hidden,
    top_logit,
    bias_logit,
):
    hosts, chips = lax.axis_size("hst"), lax.axis_size("chip")
    orphs = orphan_blocks.shape[0]
    slots = (2 * orphs + chips - 1) // chips
    owners = orphan_owner[:, 0]
    arrays = dict(
        owner=orphan_owner.T, home=resident_row_blocks, orph=orphan_blocks,
        hoff=home_offsets.transpose(1, 2, 0), ooff=orphan_offsets.transpose(0, 2, 1),
        hlen=home_lengths.T, olen=orphan_lengths, hsamp=home_samples.T, osamp=orphan_samples,
        dense=dense_inputs.T, w1=bottom_first, b1=bias_first[None], w2=bottom_second, b2=bias_second[None],
        w3=bottom_third, b3=bias_third[None], wt=top_hidden, bh=bias_hidden[None], wl=top_logit.T,
        label=labels[None],
    )
    rehomed, logits, loss, over = step(hosts, chips, slots, bias_logit, arrays)
    rehomed = lax.cond(
        over[0] > 0,
        lambda r, o, b: padded(o, b, chips, slots),
        lambda r, o, b: r,
        rehomed, owners, orphan_blocks,
    )
    rehomed, logits = finish(rehomed, logits)
    return rehomed, logits[0], loss[0]


def solution(mesh):
    both = ("hst", "chip")
    three, two = P(both, None, None), P(both, None)
    return jax.shard_map(
        per_device,
        mesh=mesh,
        in_specs=(three, three, three, two, two, three, two, two, two, two, P(both)) + (P(),) * 10,
        out_specs=(three, P(both), P()),
        check_vma=False,
    )
```

```python
import functools

import jax
import jax.numpy as jnp
from jax import lax
from jax.experimental import pallas as pl
from jax.experimental.pallas import tpu as pltpu
from jax.sharding import PartitionSpec as P

F = 26
CORES = 2
PAIR = 2
SLAB = 32
VM, HBM, SMEM = pltpu.VMEM, pltpu.HBM, pltpu.SMEM
F32, BF16, I32 = jnp.float32, jnp.bfloat16, jnp.int32
MESH = pl.DeviceIdType.MESH


def cost(flops, bytes_accessed):
    return pl.CostEstimate(flops=flops, bytes_accessed=bytes_accessed, transcendentals=0)


def nt(a, b):
    return lax.dot_general(a, b, (((1,), (1,)), ((), ())), preferred_element_type=F32)


def mm(a, b):
    return jnp.dot(a, b, preferred_element_type=F32)


def turn(j, half):
    if j >= half - CORES:
        return 0, half - 1 - j
    return 1 + j // CORES, j % CORES


def walk(chip, half, side, a, b):
    per = half // CORES
    base, local = lax.div(chip, half), lax.rem(chip, half)
    base = lax.rem(base + side, 2) * half
    return base + lax.rem(lax.div(local, CORES) + a, per) * CORES + lax.rem(local + b, CORES)


def passes(half, slots, ends):
    found = []
    for j in range(half):
        low = 0
        for k, end in enumerate(ends):
            high = slots if k == len(ends) - 1 else min(slots, end - j * slots)
            if high > low:
                found.append((k, j, low, high))
                low = high
    return sorted(found)


NAMES = (
    "owner", "orph", "home", "hoff", "ooff", "hlen", "olen", "hsamp", "osamp",
    "dense", "w1", "b1", "w2", "b2", "w3", "b3", "wt", "bh", "wl", "label",
)


def step_kernel(hosts, chips, slots, cap, depth, *refs):
    half = chips // 2
    devices = hosts * chips
    bl_ref = refs[0]
    hbm = dict(zip(NAMES, refs[1:1 + len(NAMES)]))
    refs = refs[1 + len(NAMES):]
    rehomed, logit_ref, loss_ref, over_ref = refs[:4]
    v = dict(zip(NAMES, refs[4:4 + len(NAMES)]))
    (packed, relay, held, fwd, meta_send, meta, stage, counts, rows, out_rows, arrived, pieces, slab, gram, wpad, wexp,
     order, loss_send, losses,
     in_sems, meta_s, meta_r, row_s, row_r, loss_s, loss_r, list_s, list_r, near_s, near_r, fwd_s, fwd_r) = refs[4 + len(NAMES):]

    homes, height = v["home"].shape[0], v["home"].shape[1]
    orphs = v["orph"].shape[0]
    count = homes + orphs
    total = devices * count
    width = v["home"].shape[2]
    batch = logit_ref.shape[1]
    quarter = orphs // 8
    ends = [2 * quarter, 3 * quarter, 4 * quarter, 5 * quarter, cap]
    starts = [0] + ends[:-1]
    steps = len(ends)

    host, chip = lax.axis_index("hst"), lax.axis_index("chip")
    me = host * chips + chip
    my_half = lax.div(chip, half)
    local, core = lax.div(lax.rem(chip, half), CORES), lax.rem(chip, CORES)
    low_chip = lax.div(local, PAIR) * PAIR
    gate = lax.rem(local, PAIR) == 1 - my_half
    half_chips = half // CORES
    across = (1 - my_half) * half
    target = across + (low_chip + my_half) * CORES + core
    holders = [across + (low_chip + i) * CORES + core for i in range(PAIR)]
    turn_in = lax.rem(local, PAIR)

    at_host = [lax.rem(host + dh, hosts) for dh in range(hosts)]
    at_chip = [walk(chip, half, side, k // CORES, k % CORES) for side in range(2) for k in range(half)]
    peers = [(at_host[dh], at_chip[side * half + k])
             for side in range(2) for dh in range(hosts) for k in range(half)]
    others = [(e, *peers[e]) for e in range(devices - 1, 0, -1)]

    loads = {n: pltpu.make_async_copy(hbm[n], v[n], in_sems.at[k]) for k, n in enumerate(NAMES)}
    for n in NAMES[:2]:
        loads[n].start()
    bar = pltpu.get_barrier_semaphore()

    for _, h, c in others:
        pl.semaphore_signal(bar, 1, device_id=(h, c), device_id_type=MESH)
    for n in NAMES[2:]:
        loads[n].start()

    def everyone(src, dst, send, recv, indexed):
        copies = [
            pltpu.make_async_remote_copy(
                src_ref=src.at[h * chips + c] if indexed else src.at[0],
                dst_ref=dst.at[me], send_sem=send.at[e], recv_sem=recv.at[e],
                device_id=(h, c), device_id_type=MESH)
            for e, h, c in others
        ]

        def start():
            for copy in copies:
                copy.start()

        def wait(kind):
            for copy in copies:
                copy.wait_recv() if kind == "recv" else copy.wait_send()

        return start, wait

    meta_go, meta_wait = everyone(meta_send, meta, meta_s, meta_r, True)
    rows_go, rows_wait = everyone(out_rows, arrived, row_s, row_r, True)
    loss_go, loss_wait = everyone(loss_send, losses, loss_s, loss_r, False)

    lists = [
        pltpu.make_async_remote_copy(
            src_ref=packed.at[pl.ds(half * slots + starts[k], ends[k] - starts[k])],
            dst_ref=relay.at[turn_in, pl.ds(starts[k], ends[k] - starts[k])],
            send_sem=list_s.at[k], recv_sem=list_r.at[turn_in, k],
            device_id=(host, target), device_id_type=MESH)
        for k in range(steps)
    ]

    def listed(i, k):
        size = ends[k] - starts[k]
        return pltpu.make_async_remote_copy(
            src_ref=packed.at[pl.ds(half * slots + starts[k], size)],
            dst_ref=relay.at[i, pl.ds(starts[k], size)],
            send_sem=list_s.at[k], recv_sem=list_r.at[i, k],
            device_id=(host, target), device_id_type=MESH)

    def group(src, holder, j, low, high, send, recv):
        return pltpu.make_async_remote_copy(
            src_ref=src.at[pl.ds(j * slots + low, high - low)],
            dst_ref=rehomed.at[pl.ds(holder * slots + low, high - low)],
            send_sem=send, recv_sem=recv,
            device_id=(host, walk(chip, half, 0, *turn(j, half))), device_id_type=MESH)

    near = [group(packed, chip, j, 0, slots, near_s.at[j], near_r.at[j]) for j in range(half - 1)]
    onward = {}
    for n, (k, j, low, high) in enumerate(passes(half, slots, ends)):
        for i in range(PAIR):
            if j < half - 1:
                onward[i, k, j] = group(fwd.at[i], holders[i], j, low, high, fwd_s.at[i, n], fwd_r.at[i, n])

    loads["owner"].wait()
    to = v["owner"][...]
    key = jnp.zeros_like(to)
    for side in range(2):
        for j in range(half):
            owner = walk(target if side else chip, half, 0, *turn(j, half))
            key = jnp.where(to == owner, side * half + j, key)
    tag = lax.broadcasted_iota(I32, to.shape, 1)
    square = (orphs, orphs)
    code = jnp.broadcast_to((key * orphs + tag).astype(F32), square)
    kind = jnp.broadcast_to(key.astype(F32), square)
    rank = jnp.sum((code.T < code).astype(F32), axis=0, keepdims=True).astype(I32)
    prefix = jnp.sum((kind.T < kind).astype(F32), axis=0, keepdims=True).astype(I32)
    inside = jnp.sum((kind.T < half).astype(F32), axis=0, keepdims=True).astype(I32)
    place = jnp.where(key < half, key * slots + rank - prefix, half * slots + rank - inside)
    loads["orph"].wait()

    def pack(first_at, number):
        for t in range(first_at, first_at + number):
            found = jnp.sum(jnp.where(place == t, tag + 1, 0))
            block = v["orph"][jnp.maximum(found - 1, 0)]
            packed[t] = jnp.where(found > 0, block, jnp.zeros_like(block))

    pack(half * slots, ends[0])
    pl.semaphore_wait(bar, devices - 1)
    lists[0].start()
    sizes = [jnp.sum((key == half + j).astype(I32)) for j in range(half)]
    sizes.append(jnp.sum((key >= half).astype(I32)))
    stage[...] = jnp.zeros_like(stage)
    loads["osamp"].wait()
    stage[0:orphs, 0:devices] = v["osamp"][...].astype(F32)
    turned = stage[...].T[0:devices].astype(I32)
    lane = lax.broadcasted_iota(I32, (devices, 128), 1)
    rest = pltpu.roll(turned, homes, 1)
    loads["hsamp"].wait()
    stage[0:devices, 0:homes] = v["hsamp"][...].astype(F32)
    line = jnp.where(lane < homes, stage[0:devices].astype(I32), rest)
    for j in range(half + 1):
        line = jnp.where(lane == count + j, sizes[j], line)
    for p in range(devices):
        meta_send[p] = line[p:p + 1]
    meta[me] = meta_send[me]

    meta_go()

    pack(0, half * slots)
    near[0].start()

    @pl.when(gate)
    def _():
        for j in range(1, half - CORES):
            near[j].start()

    for j in range(half - CORES, half - 1):
        near[j].start()
    rehomed[pl.ds(chip * slots, slots)] = packed[(half - 1) * slots:half * slots]
    pack(half * slots + starts[1], cap - starts[1])

    row = lax.broadcasted_iota(I32, (height, 128), 0)
    bag = hbm["hoff"].shape[1]

    def hits(off):
        found = jnp.zeros((height, 128), F32)
        for k in range(bag):
            found = found + (row == off[k:k + 1]).astype(F32)
        return found.T

    for n in ("hoff", "hlen"):
        loads[n].wait()
    slot = lax.broadcasted_iota(I32, (bag, homes), 0)
    blank = jnp.full((bag, 64 - homes), height, I32)

    def pair(g, carry):
        off = []
        for k in range(2):
            p = g * 2 + k
            off += [jnp.where(slot < v["hlen"][pl.ds(p, 1), :], v["hoff"][p], height), blank]
        found = hits(jnp.concatenate(off, axis=1))
        for k in range(2):
            counts[pl.ds(pl.multiple_of((g * 2 + k) * homes, 8), homes), :] = found[k * 64:k * 64 + homes]
        return carry

    lax.fori_loop(0, devices // 2, pair, 0)
    loads["home"].wait()

    def home_piece(b, carry):
        lhs = counts[pl.ds(b, devices, stride=homes), :].astype(BF16)
        rows[pl.ds(b, devices, stride=count), :] = mm(lhs, v["home"][b])
        return carry

    lax.fori_loop(0, homes, home_piece, 0, unroll=4)
    for n in ("ooff", "olen"):
        loads[n].wait()
    per = 128 // devices
    spot = lax.broadcasted_iota(I32, (bag, devices), 0)

    def orph_group(g, carry):
        off = []
        for k in range(per):
            b = g * per + k
            off.append(jnp.where(spot < v["olen"][pl.ds(b, 1), :], v["ooff"][b], height))
        found = hits(jnp.concatenate(off, axis=1) if per > 1 else off[0]).astype(BF16)
        for k in range(per):
            b = g * per + k
            rows[pl.ds(homes + b, devices, stride=count), :] = mm(found[k * devices:(k + 1) * devices], v["orph"][b])
        return carry

    lax.fori_loop(0, orphs // per, orph_group, 0)
    out_rows[...] = rows[...].reshape(out_rows.shape).astype(BF16)
    rows_go()

    arrived[me] = out_rows[me]

    for n in NAMES[9:]:
        loads[n].wait()
    inter = v["wt"].shape[0]
    whole = inter // 16 * 16
    wpad[whole:, :] = jnp.zeros((wpad.shape[0] - whole, wpad.shape[1]), BF16)
    wpad[0:inter, :] = v["wt"][...]
    cell = lax.broadcasted_iota(I32, (SLAB * SLAB, wpad.shape[0]), 0)
    i, j = cell // SLAB, cell % SLAB
    column = lax.broadcasted_iota(I32, cell.shape, 1)
    pick = (column == 128 + i * (i - 1) // 2 + j) & (j < i) & (i <= F)
    wexp[...] = mm(jnp.where(pick, 1.0, 0.0).astype(BF16), wpad[...]).astype(BF16)

    first = lax.dot_general(v["dense"][...], v["w1"][...], (((0,), (0,)), ((), ())), preferred_element_type=F32)
    first = jnp.maximum(first + v["b1"][...], 0.0).astype(BF16)
    second = jnp.maximum(mm(first, v["w2"][...]) + v["b2"][...], 0.0).astype(BF16)
    slab[0] = jnp.maximum(mm(second, v["w3"][...]) + v["b3"][...], 0.0)
    slab[F + 1:] = jnp.zeros((SLAB - F - 1,) + slab.shape[1:], F32)

    meta_wait("recv")
    def unpack(k):
        size = ends[k] - starts[k]
        for i in range(PAIR):
            listed(i, k).wait_recv()
            held[i, starts[k]:ends[k]] = relay[i, starts[k]:ends[k]]
            bits = meta[host * chips + holders[i]]
            here = lax.broadcasted_iota(I32, bits.shape, 1)
            for step_, j, low, high in passes(half, slots, ends):
                if step_ != k:
                    continue
                first_at = jnp.sum(jnp.where((here >= count) & (here < count + j), bits, 0))
                number = jnp.sum(jnp.where(here == count + j, bits, 0))

                def go(s, carry):
                    at = jnp.minimum(first_at + s, cap - 1)
                    block = held[i, at]
                    block = jnp.where(s < number, block, jnp.zeros_like(block))
                    if j < half - 1:
                        fwd[i, j * slots + s] = block
                    else:
                        rehomed[holders[i] * slots + s] = block
                    return carry

                lax.fori_loop(low, high, go, 0)
                if j < half - 1:
                    onward[i, k, j].start()

    at_lane = lax.broadcasted_iota(I32, (1, 128), 1)
    for d in range(depth):
        values = jnp.full((1, 128), -1, I32)
        n = d * F
        while n < min((d + 1) * F, total):
            if n < devices * homes:
                p, s = n // homes, n % homes
                size = homes - s
            else:
                p, s = (n - devices * homes) // orphs, (n - devices * homes) % orphs
                size = orphs - s
                s = homes + s
            to = n - d * F
            size = min(size, F - to)
            moved = pltpu.roll(meta[p], (to - s) % 128, 1) if to != s else meta[p]
            values = jnp.where((at_lane >= to) & (at_lane < to + size), moved, values)
            n += size
        order[d:d + 1, :] = values.astype(F32)
    where = order[...].T[0:SLAB].astype(I32)

    @pl.when(gate)
    def _():
        unpack(0)

    pieces[total:, :] = jnp.zeros((pieces.shape[0] - total, pieces.shape[1]), F32)
    rows_wait("recv")

    lists[1].start()
    lists[2].start()
    lists[3].start()

    @pl.when(jnp.logical_not(gate))
    def _():
        for j in range(1, half - CORES):
            near[j].start()

    def settle(p, carry):
        pieces[pl.ds(pl.multiple_of(p * homes, 8), homes), :] = arrived[p, 0:homes].astype(F32)
        pieces[pl.ds(pl.multiple_of(devices * homes + p * orphs, 8), orphs), :] = (
            arrived[p, homes:count].astype(F32))
        return carry

    lax.fori_loop(0, devices, settle, 0, unroll=2)

    sample = lax.broadcasted_iota(I32, (batch, depth), 0)
    for f in range(F):
        mine = pieces[pl.ds(f, depth, stride=F), :].astype(BF16)
        hot = jnp.where(sample == where[f:f + 1, :], 1.0, 0.0).astype(BF16)
        slab[f + 1] = mm(hot, mine)

    edge = SLAB * 8
    same = (lax.broadcasted_iota(I32, (edge, edge), 0) % 8) == (
        lax.broadcasted_iota(I32, (edge, edge), 1) % 8)

    def products(g, carry):
        halves = []
        for k in range(2):
            at = pl.ds(pl.multiple_of(g * 16 + k * 8, 8), 8)
            x = slab[:, at, :].reshape(edge, slab.shape[2]).astype(BF16)
            halves.append(jnp.where(same, nt(x, x), 0.0).reshape(SLAB, 8, edge))
        both = jnp.concatenate(halves, axis=1).astype(BF16)
        gram[:, pl.ds(pl.multiple_of(g * 16, 16), 16), :] = both
        return carry

    lax.fori_loop(0, batch // 16, products, 0, unroll=2)

    @pl.when(gate)
    def _():
        unpack(1)

    lane_j = lax.broadcasted_iota(I32, (edge, edge), 0) // 8
    out_lane = lax.broadcasted_iota(I32, (edge, edge), 1)
    features = []
    for h in range(SLAB // 8):
        acc = None
        for k in range(8):
            i_ = h * 8 + k
            if i_ < 1 or i_ > F:
                continue
            live = 128 if i_ <= 16 else edge
            fold_ = jnp.where(lane_j + k * SLAB == out_lane, 1.0, 0.0).astype(BF16)
            term = mm(gram[i_, :, 0:live], fold_[0:live])
            acc = term if acc is None else acc + term
        features.append(acc.astype(BF16))
    bottom = slab[0].astype(BF16)

    tally = jnp.zeros((batch, 128), F32)
    step = 256
    scale = v["wl"][...].astype(F32)
    for n in range(0, wpad.shape[1], step):
        pre = mm(bottom, wpad[0:128, n:n + step])
        for h in range(SLAB // 8):
            pre = pre + mm(features[h], wexp[h * 256:(h + 1) * 256, n:n + step])
        hidden = jnp.maximum(pre + v["bh"][:, n:n + step], 0.0).astype(BF16).astype(F32)
        scaled = hidden * scale[:, n:n + step]
        tally = tally + scaled[:, 0:128] + scaled[:, 128:256]
    logits = jnp.sum(tally.T, axis=0, keepdims=True) + bl_ref[0]
    logit_ref[...] = logits
    soft = jnp.maximum(logits, 0.0) + jnp.log1p(jnp.exp(-jnp.abs(logits)))
    loss = jnp.sum(soft - v["label"][...].astype(F32) * logits, axis=1, keepdims=True)
    loss_send[0] = jnp.broadcast_to(loss, (1, 128))
    losses[me] = loss_send[0]
    loss_go()
    lists[4].start()

    @pl.when(gate)
    def _():
        unpack(2)
        unpack(3)
        unpack(4)

    crossing = jnp.where(at_lane == count + half, jnp.max(meta[...].astype(F32), axis=0), 0.0)
    over_ref[0] = (jnp.max(crossing) > cap).astype(I32)
    loss_wait("recv")
    loss_ref[0] = jnp.sum(jnp.where(at_lane == 0, jnp.sum(losses[...], axis=0), 0.0))

    meta_wait("send")
    rows_wait("send")
    loss_wait("send")
    for c in lists:
        c.wait_send()
    for c in near:
        c.wait()

    @pl.when(gate)
    def _():
        for k, j, low, high in passes(half, slots, ends):
            for i in range(PAIR if j < half - 1 else 0):
                onward[i, k, j].wait_send()

    for k, j, low, high in passes(half, slots, ends):
        if j == half - 1:
            continue
        source = lax.rem(local - turn(j, half)[0] + half_chips, half_chips)

        @pl.when(lax.rem(source, PAIR) == 1 - my_half)
        def _():
            for i in range(PAIR):
                onward[i, k, j].wait_recv()


def step(hosts, chips, slots, bl, arrays):
    devices = hosts * chips
    half = chips // 2
    home, orph = arrays["home"], arrays["orph"]
    homes, height, width = home.shape
    orphs = orph.shape[0]
    count = homes + orphs
    batch = arrays["dense"].shape[1]
    top = arrays["wt"].shape[1]
    cap = -(-24 * orphs // 32)
    total = devices * count
    depth = -(-total // (F * 128)) * 128
    dma = pltpu.SemaphoreType.DMA
    scratch = [VM(arrays[n].shape, arrays[n].dtype) for n in NAMES] + [
        VM((half * slots + cap, height, width), BF16),
        VM((PAIR, cap, height, width), BF16),
        VM((PAIR, cap, height, width), BF16),
        VM((PAIR, half * slots, height, width), BF16),
        VM((devices, 1, 128), I32),
        VM((devices, 1, 128), I32),
        VM((128, 128), F32),
        VM((devices * homes, height), F32),
        VM((devices * count, width), F32),
        VM((devices, count, width), BF16),
        VM((devices, count, width), BF16),
        VM((F * depth, width), F32),
        VM((SLAB, batch, width), F32),
        VM((SLAB, batch, SLAB * 8), BF16),
        VM((512, top), BF16),
        VM((SLAB * SLAB, top), BF16),
        VM((depth, 128), F32),
        VM((1, 1, 128), F32),
        VM((devices, 1, 128), F32),
        dma((len(NAMES),)),
        dma((devices,)), dma((devices,)), dma((devices,)), dma((devices,)), dma((devices,)), dma((devices,)),
        dma((5,)), dma((PAIR, 5)),
        dma((half,)), dma((half,)), dma((PAIR, 2 * half + 5)), dma((PAIR, 2 * half + 5)),
    ]
    smem, hbm, vmem = (pl.BlockSpec(memory_space=m) for m in (SMEM, HBM, VM))
    return pl.pallas_call(
        functools.partial(step_kernel, hosts, chips, slots, cap, depth),
        out_shape=(
            jax.ShapeDtypeStruct((chips * slots, height, width), BF16),
            jax.ShapeDtypeStruct((1, batch), F32),
            jax.ShapeDtypeStruct((1,), F32),
            jax.ShapeDtypeStruct((1,), I32),
        ),
        in_specs=[smem] + [hbm] * len(NAMES),
        out_specs=(vmem, vmem, smem, smem),
        scratch_shapes=scratch,
        cost_estimate=cost(8_000_000_000, 8_000_000),
        compiler_params=pltpu.CompilerParams(
            collective_id=0, has_side_effects=True, vmem_limit_bytes=56 * 2**20),
        name="step",
    )(bl, *[arrays[n] for n in NAMES])


def finish_kernel(parts, rehomed, logits, rehomed_out, logits_out, sems):
    size = rehomed.shape[0] // parts
    copies = [
        pltpu.make_async_copy(rehomed.at[pl.ds(k * size, size)], rehomed_out.at[pl.ds(k * size, size)], sems.at[k])
        for k in range(parts)
    ]
    copies.append(pltpu.make_async_copy(logits, logits_out, sems.at[parts]))
    for copy in copies:
        copy.start()
    for copy in copies:
        copy.wait()


def finish(rehomed, logits, parts=4):
    vmem, hbm = pl.BlockSpec(memory_space=VM), pl.BlockSpec(memory_space=HBM)
    return pl.pallas_call(
        functools.partial(finish_kernel, parts),
        out_shape=(jax.ShapeDtypeStruct(rehomed.shape, rehomed.dtype),
                   jax.ShapeDtypeStruct(logits.shape, logits.dtype)),
        in_specs=[vmem, pl.BlockSpec(memory_space=pl.ANY)],
        out_specs=(hbm, hbm),
        scratch_shapes=[pltpu.SemaphoreType.DMA((parts + 1,))],
        cost_estimate=cost(1000, 2 * rehomed.size * 2),
        compiler_params=pltpu.CompilerParams(vmem_limit_bytes=2 * 2**20),
        name="finish",
    )(rehomed, logits)


def padded(owners, blocks, chips, slots):
    number = blocks.shape[0]
    index = jnp.arange(number, dtype=I32)
    earlier = index[None, :] < index[:, None]
    rank = jnp.sum(((owners[:, None] == owners[None, :]) & earlier).astype(I32), axis=1)
    match = (owners * slots + rank)[None, :] == jnp.arange(chips * slots, dtype=I32)[:, None]
    source = jnp.sum(match.astype(I32) * index[None, :], axis=1)
    filled = jnp.any(match, axis=1)
    groups = jnp.where(filled[:, None, None], blocks[source], jnp.zeros((), BF16))
    return lax.all_to_all(groups, "chip", split_axis=0, concat_axis=0, tiled=True)


def per_device(
    resident_row_blocks,
    orphan_blocks,
    home_offsets,
    home_lengths,
    home_samples,
    orphan_offsets,
    orphan_lengths,
    orphan_samples,
    orphan_owner,
    dense_inputs,
    labels,
    bottom_first,
    bias_first,
    bottom_second,
    bias_second,
    bottom_third,
    bias_third,
    top_hidden,
    bias_hidden,
    top_logit,
    bias_logit,
):
    hosts, chips = lax.axis_size("hst"), lax.axis_size("chip")
    orphs = orphan_blocks.shape[0]
    slots = (2 * orphs + chips - 1) // chips
    owners = orphan_owner[:, 0]
    arrays = dict(
        owner=orphan_owner.T, home=resident_row_blocks, orph=orphan_blocks,
        hoff=home_offsets.transpose(1, 2, 0), ooff=orphan_offsets.transpose(0, 2, 1),
        hlen=home_lengths.T, olen=orphan_lengths, hsamp=home_samples.T, osamp=orphan_samples,
        dense=dense_inputs.T, w1=bottom_first, b1=bias_first[None], w2=bottom_second, b2=bias_second[None],
        w3=bottom_third, b3=bias_third[None], wt=top_hidden, bh=bias_hidden[None], wl=top_logit.T,
        label=labels[None],
    )
    rehomed, logits, loss, over = step(hosts, chips, slots, bias_logit, arrays)
    rehomed = lax.cond(
        over[0] > 0,
        lambda r, o, b: padded(o, b, chips, slots),
        lambda r, o, b: r,
        rehomed, owners, orphan_blocks,
    )
    rehomed, logits = finish(rehomed, logits)
    return rehomed, logits[0], loss[0]


def solution(mesh):
    both = ("hst", "chip")
    three, two = P(both, None, None), P(both, None)
    return jax.shard_map(
        per_device,
        mesh=mesh,
        in_specs=(three, three, three, two, two, three, two, two, two, two, P(both)) + (P(),) * 10,
        out_specs=(three, P(both), P()),
        check_vma=False,
    )
```
